512 devices in a mesh: band: 16 (over y, core), aperture: 32 (over x, z).
Axes of the slice: x: 4, y: 8, z: 8, core: 2. Of those that a mesh axis runs over, the one named last changes fastest.
Arguments:
- raw_echoes: bfloat16 [16384, 2, 4096], P('aperture', None, 'band'), may hold values from -6 to 6
- pulse_order: int32 [32, 16, 32], P('aperture', 'band'), may hold values from 0 to 31, each once within a row
- matched: float32 [2, 4096], replicated, may hold values from -6 to 6
- offsets: int32 [14, 2, 2, 1], replicated, may hold values from 0 to 16
- fraction: float32 [14, 2, 2], replicated, may hold values from 0 to 0.4
- tilt_angle: float32 [14, 2], replicated, may hold values from -3.140625 to 3.140625
Outputs:
- speckle_image: float32 [16384, 128], P(('band', 'aperture'))
The draws below stay inside these ranges and needn't reach their ends.
Inputs may be any that keep to these rules, and one draw needn't show every extreme that they name: `pulse_order`: each row of 32 entries names every number below 32 once.
All inputs are finite; a program needn't handle non-finite values.
Results may differ from the reference program's by a relative error of at most 0.0025.
Values may be sent and summed in bfloat16 or wider, within the bound.
A program may use at most 64 MiB of HBM per device.

```python
import math
import jax
import jax.numpy as jnp
from jax import lax

FREQ = 4096
R = 128
LOCAL_LEV = 5
SHIFT = 8
PUL_DEV = 32
NBD = 16
NAP = 32
LEVELS = 14
PULSES = 16384
RBLK = 1
N_BAND = 16
N_APERTURE = 32


def touch_ends(values, own_key, least, top_value):
    spot = [jax.random.randint(jax.random.fold_in(own_key, axis), (), 0, length) for axis, length in enumerate(values.shape)]
    longest = values.shape.index(max(values.shape))
    next_to = spot[:longest] + [(spot[longest] + 1) % values.shape[longest]] + spot[longest + 1:]
    return values.at[tuple(spot)].set(least).at[tuple(next_to)].set(top_value)


def steps_of(stream_key, extent, split, low, high):
    def one(axis_at, shards_of):
        steps = jax.random.uniform(jax.random.fold_in(jax.random.fold_in(stream_key, 6), axis_at), (shards_of,), jnp.float32, low / len(split), high / len(split))
        return jnp.repeat(jnp.exp(steps), extent[axis_at] // shards_of).reshape((-1,) + (1,) * (len(extent) - axis_at - 1))

    level = one(*split[0])
    for cut in split[1:]:
        level = level * one(*cut)
    return level


def normal_values(key, extent, scale, limit, pieces=(), kind=jnp.bfloat16):
    result = scale * jax.random.normal(key, extent, jnp.float32)
    if pieces:
        result = result * steps_of(key, extent, pieces, -0.22, 0.18)
    return jnp.clip(result, -limit, limit).astype(kind)


def setup_inputs(seed: int = 0) -> dict:
    streams_of = jax.random.split(jax.random.key(seed), 7)
    raw_echoes = normal_values(streams_of[0], (PULSES, 2, FREQ), 1.0, 6.0, ((0, 32), (2, 16)))
    pulse_order = jax.vmap(lambda own: jax.random.permutation(own, PUL_DEV))(jax.random.split(streams_of[1], NAP * NBD)).reshape((NAP, NBD, PUL_DEV)).astype(jnp.int32)
    matched = normal_values(streams_of[2], (2, FREQ), 1.0, 6.0, (), jnp.float32)
    offsets = touch_ends(jax.random.randint(streams_of[3], (LEVELS, 2, 2, RBLK), 0, 2 * SHIFT + 1), jax.random.fold_in(streams_of[3], 1), 0, 2 * SHIFT).astype(jnp.int32)
    fraction = jnp.clip(jax.random.uniform(streams_of[4], (LEVELS, 2, 2), jnp.float32, 0.0, 0.4), 0.0, 0.4)
    tilt_angle = jnp.clip(jax.random.uniform(streams_of[5], (LEVELS, 2), jnp.float32, -3.140625, 3.140625), -3.140625, 3.140625)
    return {"raw_echoes": raw_echoes, "pulse_order": pulse_order, "matched": matched, "offsets": offsets, "fraction": fraction, "tilt_angle": tilt_angle}


HIGHEST = lax.Precision.HIGHEST

def range_table(matched_part, freq_start, bin_start, bin_count):
    freq_count = matched_part.shape[1]
    freq_index = freq_start + jnp.arange(freq_count, dtype=jnp.int32)
    bin_index = bin_start + jnp.arange(bin_count, dtype=jnp.int32)
    phase_turns = freq_index[:, None] * bin_index[None, :] % FREQ
    phase_angle = phase_turns.astype(jnp.float32) * (2.0 * math.pi / FREQ)
    cosine = jnp.cos(phase_angle)
    sine_part = jnp.sin(phase_angle)
    spec_real = matched_part[0][:, None]
    spec_imag = matched_part[1][:, None]
    norm_scale = 1.0 / math.sqrt(FREQ)
    table_real = (spec_real * cosine - spec_imag * sine_part) * norm_scale
    table_imag = (spec_real * sine_part + spec_imag * cosine) * norm_scale
    upper_rows = jnp.concatenate([table_real, table_imag], axis=1)
    lower_rows = jnp.concatenate([-table_imag, table_real], axis=1)
    return jnp.concatenate([upper_rows, lower_rows], axis=0).astype(jnp.bfloat16)

def interp_kernel(shift_frac):
    in_pos = jnp.arange(128, dtype=jnp.float32)[:, None]
    out_pos = jnp.arange(128, dtype=jnp.float32)[None, :]
    distance = in_pos - out_pos - shift_frac
    tapered = jnp.sinc(distance) * jnp.exp(-(distance / 2.5) ** 2)
    return jnp.where(jnp.abs(distance) <= 4.0, tapered, jnp.zeros_like(tapered))

def merge_pair(first_child, second_child, tree_level, beam_start, offsets, fraction, tilt_angle):
    sub_count = first_child.shape[0]
    row_count = first_child.shape[1]
    range_width = first_child.shape[3]
    block_count = range_width // 128
    halves = []
    for parity in range(2):
        beam_index = (beam_start + 2 * jnp.arange(row_count, dtype=jnp.int32) + parity).astype(jnp.float32)
        position = 2.0 * (beam_index + 0.5) / 2.0 ** (tree_level + 1) - 1.0
        summed = jnp.zeros(first_child.shape, jnp.float32)
        for child_index, child_image in enumerate((first_child, second_child)):
            padded = jnp.pad(child_image, ((0, 0), (0, 0), (0, 0), (SHIFT, SHIFT)))
            windows = []
            for block_index in range(block_count):
                start_cell = (block_index * 128 + offsets[tree_level, child_index, parity, block_index]).astype(jnp.int32)
                windows.append(lax.dynamic_slice_in_dim(padded, start_cell, 128, 3))
            stacked = jnp.stack(windows, axis=3)
            kernel = interp_kernel(fraction[tree_level, child_index, parity])
            shifted = jnp.einsum('nrckw,wo->nrcko', stacked, kernel, precision=HIGHEST)
            shifted = shifted.reshape(first_child.shape)
            phase_angle = tilt_angle[tree_level, child_index] * position
            cosine = jnp.cos(phase_angle)[None, :, None]
            sine_part = jnp.sin(phase_angle)[None, :, None]
            real_part = shifted[:, :, 0]
            imag_part = shifted[:, :, 1]
            summed = summed + jnp.stack([real_part * cosine - imag_part * sine_part, real_part * sine_part + imag_part * cosine], axis=2)
        halves.append(summed * (1.0 / math.sqrt(2.0)))
    parent = jnp.stack(halves, axis=2)
    return parent.reshape(sub_count, 2 * row_count, 2, range_width)

def box_sum(values):
    row_count = values.shape[1]
    range_width = values.shape[2]
    padded = jnp.pad(values, ((0, 0), (2, 2), (2, 2)))
    across = padded[:, 0:row_count, :]
    for offset_row in range(1, 5):
        across = across + padded[:, offset_row:offset_row + row_count, :]
    summed = across[:, :, 0:range_width]
    for offset_col in range(1, 5):
        summed = summed + across[:, :, offset_col:offset_col + range_width]
    return summed

def speckle(intensity):
    cell_count = box_sum(jnp.ones(intensity.shape, jnp.float32))
    local_mean = box_sum(intensity) / cell_count
    local_square = box_sum(intensity * intensity) / cell_count
    lee_gain = (local_square - local_mean * local_mean) / (local_square - 0.75 * local_mean * local_mean + 0.001)
    return local_mean + lee_gain * (intensity - local_mean)

def reference(raw_echoes, pulse_order, matched, offsets, fraction, tilt_angle):
    group_count = N_BAND * N_APERTURE
    pulse_rows = (jnp.arange(group_count, dtype=jnp.int32)[:, None] * PUL_DEV + pulse_order.reshape(group_count, PUL_DEV).astype(jnp.int32)).reshape(-1)
    echoes = raw_echoes[pulse_rows].reshape(group_count, PUL_DEV, 2 * FREQ)
    dft_table = range_table(matched, 0, 0, R).astype(jnp.float32)

    def compress(group_echoes):
        return jnp.dot(group_echoes.astype(jnp.float32), dft_table, precision=HIGHEST)
    profiles = lax.map(compress, echoes)
    images = profiles.reshape(PULSES, 1, 2, R)
    for tree_level in range(LEVELS):
        images = merge_pair(images[0::2], images[1::2], tree_level, 0, offsets, fraction, tilt_angle)
    final_image = images[0]
    intensity = final_image[:, 0] ** 2 + final_image[:, 1] ** 2
    filtered = speckle(intensity.reshape(group_count, PUL_DEV, R))
    tile_index = jnp.arange(group_count, dtype=jnp.int32)
    source = tile_index % N_APERTURE * N_BAND + tile_index // N_APERTURE
    cross_bits = LEVELS - LOCAL_LEV
    reversed_index = jnp.zeros_like(source)
    for bit_index in range(cross_bits):
        reversed_index = reversed_index + source // 2 ** bit_index % 2 * 2 ** (cross_bits - 1 - bit_index)
    return filtered[reversed_index].reshape(PULSES, R)
```

```python
import functools
import math

import jax
import jax.numpy as jnp
from jax import lax
from jax.experimental import pallas as pl
from jax.experimental.pallas import tpu as pltpu
from jax.sharding import PartitionSpec as P

LEVELS = 14
F32 = jnp.float32
BF16 = jnp.bfloat16
MESH = pl.DeviceIdType.MESH


def bit_reversed(value, bits):
    return sum(((value >> t) & 1) << (bits - 1 - t) for t in range(bits))


def sin_cos(angle):
    turns = jnp.floor(angle * (2.0 / math.pi) + 0.5)
    rest = (angle - turns * 1.5707964) - turns * (-4.371139e-08)
    sq = rest * rest
    sine = rest + rest * sq * (
        -1.0 / 6 + sq * (1.0 / 120 + sq * (-1.0 / 5040 + sq * (1.0 / 362880)))
    )
    cosine = 1.0 + sq * (-0.5 + sq * (1.0 / 24 + sq * (-1.0 / 720 + sq * (1.0 / 40320))))
    size = jnp.abs(turns)
    odd = size == 1.0
    flip = jnp.where(size == 2.0, -1.0, 1.0)
    return (
        jnp.where(odd, turns * cosine, flip * sine),
        jnp.where(odd, -turns * sine, flip * cosine),
    )


def iota(shape, dim):
    return lax.broadcasted_iota(jnp.int32, shape, dim)


def bf16_pair(value):
    high = value.astype(BF16)
    low = (value - high.astype(F32)).astype(BF16)
    return high, low


def kernel(
    x_hbm, order_ref, matched_ref, offs_ref, frac_ref, tilt_ref, out_ref,
    xv, table, prods, own, other, from_core, partial, blocks,
    taps, phases, held, beams_out, beams_in, rows_out, rows_in, padded,
    x_sem, core_send, core_recv, blk_send, blk_recv, beam_send, beam_recv, row_send, row_recv,
):
    band = lax.axis_index("band")
    aperture = lax.axis_index("aperture")
    parity_word = band | (aperture << 4)
    child_word = parity_word << 5

    loads = []
    for pos in range(16):
        rel = 2 * pos + 1 if pos < 8 else 2 * (pos - 8)
        load = pltpu.make_async_copy(x_hbm.at[band ^ rel], xv.at[pos], x_sem.at[pos])
        load.start()
        loads.append(load)

    barrier = pltpu.get_barrier_semaphore()
    for rel in range(1, 16):
        pl.semaphore_signal(barrier, 1, device_id={"band": band ^ rel}, device_id_type=MESH)
    for rel in range(1, 32):
        pl.semaphore_signal(barrier, 1, device_id={"aperture": aperture ^ rel}, device_id_type=MESH)

    bins = iota((128, 128), 0).astype(F32)
    for half in range(2):
        start = pl.multiple_of(band * 256 + 128 * half, 128)
        freq = (start + iota((128, 128), 1)).astype(F32)
        turns = freq * bins
        turns = turns - 4096.0 * jnp.floor(turns * (1.0 / 4096) + 0.5)
        sine, cosine = sin_cos(turns * (2.0 * math.pi / 4096))
        spec_re = matched_ref[0:1, pl.ds(start, 128)]
        spec_im = matched_ref[1:2, pl.ds(start, 128)]
        real = (spec_re * cosine - spec_im * sine) * (1.0 / 64)
        imag = (spec_re * sine + spec_im * cosine) * (1.0 / 64)
        table[2 * half, 0:128] = real.astype(BF16)
        table[2 * half, 128:256] = imag.astype(BF16)
        table[2 * half + 1, 0:128] = (-imag).astype(BF16)
        table[2 * half + 1, 128:256] = real.astype(BF16)

    for chunk in range(4):
        for pos in range(4 * chunk, 4 * chunk + 4):
            loads[pos].wait()
        echoes = xv[4 * chunk : 4 * chunk + 4].reshape(512, 128)
        for kind in range(4):
            prod = lax.dot_general(
                echoes, table[kind], (((1,), (1,)), ((), ())), preferred_element_type=F32
            )
            prods[kind, 0] = prod[:, 0:128]
            prods[kind, 1] = prod[:, 128:256]
        target = other if chunk < 2 else own
        base = 4 * (chunk % 2)
        for part in range(2):
            total = prods[0, part, pl.ds(0, 128, stride=4), :]
            for kind in range(1, 4):
                total = total + prods[kind, part, pl.ds(kind, 128, stride=4), :]
            target[base : base + 4, :, 128 * part : 128 * part + 128] = total.reshape(4, 32, 128)

    pl.semaphore_wait(barrier, 46)

    order_far = (4, 3, 5, 2, 6, 7, 1, 0)
    core_copies = {}
    for j in order_far:
        copy = pltpu.make_async_remote_copy(
            src_ref=other.at[j], dst_ref=from_core.at[j],
            send_sem=core_send.at[j], recv_sem=core_recv.at[j],
            device_id={"band": band ^ 1}, device_id_type=MESH,
        )
        copy.start()
        core_copies[j] = copy
    blk_copies = []
    for j in order_far:
        core_copies[j].wait_recv()
        summed = (own[j] + from_core[j]).astype(BF16)
        if j == 0:
            blocks[0] = summed
            continue
        partial[j] = summed
        copy = pltpu.make_async_remote_copy(
            src_ref=partial.at[j], dst_ref=blocks.at[j],
            send_sem=blk_send.at[j], recv_sem=blk_recv.at[j],
            device_id={"band": band ^ (2 * j)}, device_id_type=MESH,
        )
        copy.start()
        blk_copies.append(copy)

    lane = iota((8, 128), 1)
    signed_lane = jnp.where(lane < 64, lane, lane - 128)
    lane8 = lane
    row8 = iota((8, 128), 0)

    @pl.loop(0, LEVELS)
    def _(level):
        parity_flip = (parity_word >> level) & 1
        child_flip = (child_word >> level) & 1
        for child in range(2):
            for half in range(2):
                offset = offs_ref[child ^ child_flip, half ^ parity_flip, 0, level]
                shift = frac_ref[child ^ child_flip, half ^ parity_flip, level]
                whole = 8 - offset - signed_lane
                dist = whole.astype(F32) - shift
                fracs = jnp.full((8, 128), math.pi, F32) * shift
                sq = fracs * fracs
                sine = fracs * (1.0 + sq * (-1.0 / 6 + sq * (1.0 / 120 + sq * (-1.0 / 5040 + sq * (1.0 / 362880 - sq * (1.0 / 39916800))))))
                sine = jnp.where((whole & 1) == 0, -sine, sine)
                zero = dist == 0.0
                sinc = jnp.where(zero, 1.0, sine / jnp.where(zero, 1.0, dist * math.pi))
                scaled = dist * (1.0 / 2.5)
                weight = sinc * jnp.exp(-(scaled * scaled)) * math.sqrt(0.5)
                weight = jnp.where(jnp.abs(dist) <= 4.0, weight, 0.0)
                strips = []
                for strip in range(16):
                    turned = pltpu.roll(weight, 8 * strip, 1, stride=1, stride_axis=0)
                    source = row8 + 8 * strip
                    window = source + 8 - offset
                    keep = (jnp.abs(lane8 - source) < 64) & (window >= 0) & (window < 128)
                    strips.append(jnp.where(keep, turned, 0.0))
                matrix = jnp.concatenate(strips, axis=0)
                high, low = bf16_pair(matrix)
                taps[level, child, 0:128, 128 * half : 128 * half + 128] = high
                taps[level, child, 128:256, 128 * half : 128 * half + 128] = low

    index = iota((32, 128), 0)
    row = index & 15
    half_bit = index >> 4
    for level in range(LEVELS):
        beam = half_bit ^ ((parity_word >> level) & 1)
        for t in range(level):
            if level <= 4 or (level <= 8 and t >= 4):
                bit = ((row >> (4 - level + t)) & 1) ^ ((parity_word >> t) & 1)
            elif t >= 9:
                bit = (row >> (level - 1 - t)) & 1
            else:
                bit = (parity_word >> t) & 1
            beam = beam + (bit << (level - t))
        position = 2.0 * (beam.astype(F32) + 0.5) / 2.0 ** (level + 1) - 1.0
        for child in range(2):
            angle = tilt_ref[child ^ ((child_word >> level) & 1), level] * position
            sine, cosine = sin_cos(angle)
            phases[level, child, 0] = cosine
            phases[level, child, 1] = sine

    padded[...] = jnp.zeros_like(padded)

    place = iota((32, 32), 0)
    pulse = ((place & 15) << 1) | (place >> 4)
    order = jnp.broadcast_to(order_ref[0:1, :].astype(F32), (32, 32))
    column = jnp.sum(jnp.where(iota((32, 32), 1) == pulse, order, 0.0), axis=1, keepdims=True)
    chosen = (iota((32, 256), 1) & 31).astype(F32)
    picker = jnp.where(chosen == column, 1.0, 0.0).astype(BF16)

    def merged(level, children):
        turned = []
        for child in range(2):
            high, low = bf16_pair(children[child])
            left = jnp.concatenate(
                [jnp.concatenate([high, high], axis=1), jnp.concatenate([low, low], axis=1)], axis=0
            )
            both = jnp.dot(left, taps[level, child], preferred_element_type=F32)
            shifted = both[0:32] + both[32:64]
            parts = []
            for half in range(2):
                real = shifted[0:16, 128 * half : 128 * half + 128]
                imag = shifted[16:32, 128 * half : 128 * half + 128]
                cosine = phases[level, child, 0, 16 * half : 16 * half + 16]
                sine = phases[level, child, 1, 16 * half : 16 * half + 16]
                parts.append((real * cosine - imag * sine, real * sine + imag * cosine))
            turned.append(parts)
        return [
            tuple(turned[0][half][part] + turned[1][half][part] for part in range(2))
            for half in range(2)
        ]

    def kept(parents):
        for half in range(2):
            for part in range(2):
                held[part, 16 * half : 16 * half + 16] = parents[half][part]
        return [
            jnp.concatenate([held[part, pl.ds(child, 16, stride=2), :] for part in range(2)], axis=0)
            for child in range(2)
        ]

    for copy in blk_copies:
        copy.wait_recv()
    profiles = jnp.dot(picker, blocks[...].reshape(256, 256), preferred_element_type=F32)
    children = [
        jnp.concatenate(
            [profiles[16 * c : 16 * c + 16, 0:128], profiles[16 * c : 16 * c + 16, 128:256]], axis=0
        )
        for c in range(2)
    ]
    for level in range(4):
        children = kept(merged(level, children))
    parents = merged(4, children)

    flat_out = beams_out.reshape(64, 128)
    flat_in = beams_in.reshape(64, 128)
    for half in range(2):
        for part in range(2):
            flat_out[pl.ds(2 * half + part, 16, stride=4), :] = parents[half][part]
            flat_in[2 * half + part : 2 * half + part + 1, :] = parents[half][part][0:1]
    beam_copies = []
    for rel in (8, 9, 6, 7, 10, 11, 4, 5, 12, 13, 14, 15, 2, 3, 1):
        copy = pltpu.make_async_remote_copy(
            src_ref=beams_out.at[rel], dst_ref=beams_in.at[rel],
            send_sem=beam_send.at[rel], recv_sem=beam_recv.at[rel],
            device_id={"band": band ^ rel}, device_id_type=MESH,
        )
        copy.start()
        beam_copies.append(copy)
    for copy in beam_copies:
        copy.wait_recv()
    children = [
        jnp.concatenate(
            [
                flat_in[pl.ds(4 * child + 2 * half + part, 8, stride=8), :]
                for part in range(2)
                for half in range(2)
            ],
            axis=0,
        )
        for child in range(2)
    ]
    for level in range(5, 8):
        children = kept(merged(level, children))
    parents = merged(8, children)

    flat_out = rows_out.reshape(64, 128)
    flat_in = rows_in.reshape(64, 128)
    for half in range(2):
        for part in range(2):
            flat_out[pl.ds(32 * half + part, 16, stride=2), :] = parents[half][part]
    for part in range(2):
        flat_in[part : part + 1, :] = parents[0][part][0:1]
    row_copies = []
    for rel in sorted(range(1, 32), key=lambda r: -min(r & 7, 8 - (r & 7)) - min(r >> 3, 4 - (r >> 3))):
        copy = pltpu.make_async_remote_copy(
            src_ref=rows_out.at[rel], dst_ref=rows_in.at[bit_reversed(rel, 5)],
            send_sem=row_send.at[rel], recv_sem=row_recv.at[rel],
            device_id={"aperture": aperture ^ rel}, device_id_type=MESH,
        )
        copy.start()
        row_copies.append(copy)
    for copy in row_copies:
        copy.wait_recv()
    children = [
        jnp.concatenate(
            [flat_in[pl.ds(32 * child + part, 16, stride=2), :] for part in range(2)], axis=0
        )
        for child in range(2)
    ]
    for level in range(9, 13):
        parents = merged(level, children)
        for half in range(2):
            for part in range(2):
                held[part, pl.ds(half, 16, stride=2), :] = parents[half][part]
        children = [
            jnp.concatenate([held[part, 16 * child : 16 * child + 16] for part in range(2)], axis=0)
            for child in range(2)
        ]
    parents = merged(13, children)
    for half in range(2):
        padded[pl.ds(8 + half, 16, stride=2), :] = parents[half][0] ** 2 + parents[half][1] ** 2

    middle = padded[8:40]
    sums = padded[6:38]
    squares = sums * sums
    for shift in range(1, 5):
        value = padded[6 + shift : 38 + shift]
        sums = sums + value
        squares = squares + value * value
    lanes = iota((32, 128), 1)

    def across(value):
        total = value
        for shift in (1, 2):
            total = total + jnp.where(lanes >= shift, pltpu.roll(value, shift, 1), 0.0)
            total = total + jnp.where(lanes < 128 - shift, pltpu.roll(value, 128 - shift, 1), 0.0)
        return total

    count_rows = jnp.minimum(index + 2, 31) - jnp.maximum(index - 2, 0) + 1
    count_lanes = jnp.minimum(lanes + 2, 127) - jnp.maximum(lanes - 2, 0) + 1
    count = (count_rows * count_lanes).astype(F32)
    mean = across(sums) / count
    square = across(squares) / count
    gain = (square - mean * mean) / (square - 0.75 * mean * mean + 0.001)
    out_ref[...] = mean + gain * (middle - mean)

    for copy in list(core_copies.values()) + blk_copies + beam_copies + row_copies:
        copy.wait_send()


def body(raw_echoes, pulse_order, matched, offsets, fraction, tilt_angle):
    echoes = raw_echoes.reshape(512, 2, 2, 128).transpose(0, 2, 1, 3).reshape(16, 128, 128)
    dma = pltpu.SemaphoreType.DMA
    vmem = pl.BlockSpec(memory_space=pltpu.VMEM)
    smem = pl.BlockSpec(memory_space=pltpu.SMEM)
    return pl.pallas_call(
        kernel,
        out_shape=jax.ShapeDtypeStruct((32, 128), F32),
        in_specs=[pl.BlockSpec(memory_space=pl.ANY), vmem, vmem, smem, smem, smem],
        out_specs=vmem,
        scratch_shapes=[
            pltpu.VMEM((16, 128, 128), BF16),
            pltpu.VMEM((4, 256, 128), BF16),
            pltpu.VMEM((4, 2, 512, 128), F32),
            pltpu.VMEM((8, 32, 256), F32),
            pltpu.VMEM((8, 32, 256), F32),
            pltpu.VMEM((8, 32, 256), F32),
            pltpu.VMEM((8, 32, 256), BF16),
            pltpu.VMEM((8, 32, 256), BF16),
            pltpu.VMEM((LEVELS, 2, 256, 256), BF16),
            pltpu.VMEM((LEVELS, 2, 2, 32, 128), F32),
            pltpu.VMEM((2, 32, 128), F32),
            pltpu.VMEM((16, 4, 128), F32),
            pltpu.VMEM((16, 4, 128), F32),
            pltpu.VMEM((32, 2, 128), F32),
            pltpu.VMEM((32, 2, 128), F32),
            pltpu.VMEM((48, 128), F32),
            dma((16,)), dma((8,)), dma((8,)), dma((8,)), dma((8,)),
            dma((16,)), dma((16,)), dma((32,)), dma((32,)),
        ],
        compiler_params=pltpu.CompilerParams(collective_id=0, has_side_effects=True),
    )(
        echoes,
        pulse_order.reshape(1, 32),
        matched,
        offsets.transpose(1, 2, 3, 0),
        fraction.transpose(1, 2, 0),
        tilt_angle.transpose(1, 0),
    )


def solution(mesh):
    in_specs = (P("aperture", None, "band"), P("aperture", "band", None), P(), P(), P(), P())
    out_specs = P(("band", "aperture"), None)
    return jax.shard_map(body, mesh=mesh, in_specs=in_specs, out_specs=out_specs, check_vma=False)
```

```python
import functools
import math

import jax
import jax.numpy as jnp
from jax import lax
from jax.experimental import pallas as pl
from jax.experimental.pallas import tpu as pltpu
from jax.sharding import PartitionSpec as P

LEVELS = 14
F32 = jnp.float32
BF16 = jnp.bfloat16
MESH = pl.DeviceIdType.MESH


def bit_reversed(value, bits):
    return sum(((value >> t) & 1) << (bits - 1 - t) for t in range(bits))


def sin_cos(angle):
    turns = jnp.floor(angle * (2.0 / math.pi) + 0.5)
    rest = (angle - turns * 1.5707964) - turns * (-4.371139e-08)
    sq = rest * rest
    sine = rest + rest * sq * (
        -1.0 / 6 + sq * (1.0 / 120 + sq * (-1.0 / 5040 + sq * (1.0 / 362880)))
    )
    cosine = 1.0 + sq * (-0.5 + sq * (1.0 / 24 + sq * (-1.0 / 720 + sq * (1.0 / 40320))))
    size = jnp.abs(turns)
    odd = size == 1.0
    flip = jnp.where(size == 2.0, -1.0, 1.0)
    return (
        jnp.where(odd, turns * cosine, flip * sine),
        jnp.where(odd, -turns * sine, flip * cosine),
    )


def iota(shape, dim):
    return lax.broadcasted_iota(jnp.int32, shape, dim)


def bf16_pair(value):
    high = value.astype(BF16)
    low = (value - high.astype(F32)).astype(BF16)
    return high, low


def kernel(
    x_hbm, order_hbm, matched_hbm, offs_hbm, frac_hbm, tilt_hbm, out_ref,
    order_ref, matched_ref, offs_ref, frac_ref, tilt_ref,
    xv, table, prods, own, other, from_core, partial, blocks,
    taps, phases, held, beams_out, beams_in, rows_out, rows_in, padded,
    core_ready, band_ready, all_ready, arg_sem, x_sem, core_send, core_recv, blk_send, blk_recv, beam_send, beam_recv, row_send, row_recv,
):
    band = lax.axis_index("band")
    aperture = lax.axis_index("aperture")
    parity_word = band | (aperture << 4)
    child_word = parity_word << 5

    on_first = (band & 1) == 0
    on_second = (band & 1) == 1
    speaker = band == 0
    listener = on_first & (band > 0)
    barrier = pltpu.get_barrier_semaphore()

    def greet(peer):
        pl.semaphore_signal(barrier, 1, device_id={"band": peer}, device_id_type=MESH)

    def tell(semaphore, peer):
        pl.semaphore_signal(semaphore, 1, device_id={"band": peer}, device_id_type=MESH)

    @pl.when(on_first)
    def _():
        greet(band ^ 1)

    for rel in range(2, 16, 2):
        peer = (band & 14) ^ rel

        @pl.when(peer > 0)
        def _():
            greet(peer)

    start = pl.multiple_of(band * 256, 256)
    args = [
        pltpu.make_async_copy(source, target, arg_sem.at[i])
        for i, (source, target) in enumerate(
            (
                (matched_hbm.at[:, pl.ds(start, 256)], matched_ref),
                (order_hbm, order_ref),
                (offs_hbm, offs_ref),
                (frac_hbm, frac_ref),
                (tilt_hbm, tilt_ref),
            )
        )
    ]
    args[0].start()

    loads = []
    for pos in range(16):
        rel = 2 * pos + 1 if pos < 8 else 2 * (pos - 8)
        load = pltpu.make_async_copy(x_hbm.at[band ^ rel], xv.at[pos], x_sem.at[pos])
        load.start()
        loads.append(load)
    for arg in args[1:]:
        arg.start()

    bins = iota((128, 128), 0).astype(F32)
    args[0].wait()
    for half in range(2):
        freq = (start + 128 * half + iota((128, 128), 1)).astype(F32)
        turns = freq * bins
        turns = turns - 4096.0 * jnp.floor(turns * (1.0 / 4096) + 0.5)
        sine, cosine = sin_cos(turns * (2.0 * math.pi / 4096))
        spec_re = matched_ref[0:1, 128 * half : 128 * half + 128]
        spec_im = matched_ref[1:2, 128 * half : 128 * half + 128]
        real = (spec_re * cosine - spec_im * sine) * (1.0 / 64)
        imag = (spec_re * sine + spec_im * cosine) * (1.0 / 64)
        table[2 * half, 0:128] = real.astype(BF16)
        table[2 * half, 128:256] = imag.astype(BF16)
        table[2 * half + 1, 0:128] = (-imag).astype(BF16)
        table[2 * half + 1, 128:256] = real.astype(BF16)

    def compress(chunk, target):
        for pos in range(4 * chunk, 4 * chunk + 4):
            loads[pos].wait()
        echoes = xv[4 * chunk : 4 * chunk + 4].reshape(512, 128)
        for kind in range(4):
            prod = lax.dot_general(
                echoes, table[kind], (((1,), (1,)), ((), ())), preferred_element_type=F32
            )
            prods[kind, 0] = prod[:, 0:128]
            prods[kind, 1] = prod[:, 128:256]
        base = 4 * (chunk % 2)
        for part in range(2):
            total = prods[0, part, pl.ds(0, 128, stride=4), :]
            for kind in range(1, 4):
                total = total + prods[kind, part, pl.ds(kind, 128, stride=4), :]
            target[base : base + 4, :, 128 * part : 128 * part + 128] = total.reshape(4, 32, 128)

    order_far = (4, 3, 5, 2, 6, 7, 1, 0)
    core_copies = {}

    def to_partner(slots):
        for j in slots:
            copy = pltpu.make_async_remote_copy(
                src_ref=other.at[j], dst_ref=from_core.at[j],
                send_sem=core_send.at[j], recv_sem=core_recv.at[j],
                device_id={"band": band ^ 1}, device_id_type=MESH,
            )
            copy.start()
            core_copies[j] = copy

    compress(1, other)

    @pl.when(on_second)
    def _():
        pl.semaphore_wait(barrier, 1)
        tell(core_ready, band ^ 1)

    @pl.when(on_first)
    def _():
        pl.semaphore_wait(core_ready, 1)

    to_partner((4, 5, 6, 7))
    compress(0, other)
    to_partner((3, 2, 1, 0))
    compress(3, own)
    compress(2, own)

    @pl.when(listener)
    def _():
        pl.semaphore_wait(barrier, 14)
        tell(band_ready, band ^ 1)

    @pl.when(band == 2)
    def _():
        tell(band_ready, 0)

    @pl.when(speaker)
    def _():
        pl.semaphore_wait(band_ready, 1)
        tell(band_ready, 1)
        for rel in range(1, 32):
            pl.semaphore_signal(
                barrier, 1, device_id={"aperture": aperture ^ rel}, device_id_type=MESH
            )

    @pl.when(on_second)
    def _():
        pl.semaphore_wait(band_ready, 1)

    blk_copies = []
    for j in order_far:
        core_copies[j].wait_recv()
        summed = (own[j] + from_core[j]).astype(BF16)
        if j == 0:
            blocks[0] = summed
            continue
        partial[j] = summed
        copy = pltpu.make_async_remote_copy(
            src_ref=partial.at[j], dst_ref=blocks.at[j],
            send_sem=blk_send.at[j], recv_sem=blk_recv.at[j],
            device_id={"band": band ^ (2 * j)}, device_id_type=MESH,
        )
        copy.start()
        blk_copies.append(copy)

    for arg in args[1:]:
        arg.wait()
    lane = iota((8, 128), 1)
    signed_lane = jnp.where(lane < 64, lane, lane - 128)
    lane8 = lane
    row8 = iota((8, 128), 0)

    @pl.loop(0, LEVELS)
    def _(level):
        parity_flip = (parity_word >> level) & 1
        child_flip = (child_word >> level) & 1
        for child in range(2):
            for half in range(2):
                offset = offs_ref[child ^ child_flip, half ^ parity_flip, 0, level]
                shift = frac_ref[child ^ child_flip, half ^ parity_flip, level]
                whole = 8 - offset - signed_lane
                dist = whole.astype(F32) - shift
                fracs = jnp.full((8, 128), math.pi, F32) * shift
                sq = fracs * fracs
                sine = fracs * (1.0 + sq * (-1.0 / 6 + sq * (1.0 / 120 + sq * (-1.0 / 5040 + sq * (1.0 / 362880 - sq * (1.0 / 39916800))))))
                sine = jnp.where((whole & 1) == 0, -sine, sine)
                zero = dist == 0.0
                sinc = jnp.where(zero, 1.0, sine / jnp.where(zero, 1.0, dist * math.pi))
                scaled = dist * (1.0 / 2.5)
                weight = sinc * jnp.exp(-(scaled * scaled)) * math.sqrt(0.5)
                weight = jnp.where(jnp.abs(dist) <= 4.0, weight, 0.0)
                strips = []
                for strip in range(16):
                    turned = pltpu.roll(weight, 8 * strip, 1, stride=1, stride_axis=0)
                    source = row8 + 8 * strip
                    window = source + 8 - offset
                    keep = (jnp.abs(lane8 - source) < 64) & (window >= 0) & (window < 128)
                    strips.append(jnp.where(keep, turned, 0.0))
                matrix = jnp.concatenate(strips, axis=0)
                high, low = bf16_pair(matrix)
                taps[level, child, 0:128, 128 * half : 128 * half + 128] = high
                taps[level, child, 128:256, 128 * half : 128 * half + 128] = low

    index = iota((32, 128), 0)
    row = index & 15
    half_bit = index >> 4
    for level in range(LEVELS):
        beam = half_bit ^ ((parity_word >> level) & 1)
        for t in range(level):
            if level <= 4 or (level <= 8 and t >= 4):
                bit = ((row >> (4 - level + t)) & 1) ^ ((parity_word >> t) & 1)
            elif t >= 9:
                bit = (row >> (level - 1 - t)) & 1
            else:
                bit = (parity_word >> t) & 1
            beam = beam + (bit << (level - t))
        position = 2.0 * (beam.astype(F32) + 0.5) / 2.0 ** (level + 1) - 1.0
        for child in range(2):
            angle = tilt_ref[child ^ ((child_word >> level) & 1), level] * position
            sine, cosine = sin_cos(angle)
            phases[level, child, 0] = cosine
            phases[level, child, 1] = sine

    padded[...] = jnp.zeros_like(padded)

    place = iota((32, 32), 0)
    pulse = ((place & 15) << 1) | (place >> 4)
    order = jnp.broadcast_to(order_ref[0:1, :].astype(F32), (32, 32))
    column = jnp.sum(jnp.where(iota((32, 32), 1) == pulse, order, 0.0), axis=1, keepdims=True)
    chosen = (iota((32, 256), 1) & 31).astype(F32)
    picker = jnp.where(chosen == column, 1.0, 0.0).astype(BF16)

    def merged(level, children):
        turned = []
        for child in range(2):
            high, low = bf16_pair(children[child])
            left = jnp.concatenate(
                [jnp.concatenate([high, high], axis=1), jnp.concatenate([low, low], axis=1)], axis=0
            )
            both = jnp.dot(left, taps[level, child], preferred_element_type=F32)
            shifted = both[0:32] + both[32:64]
            parts = []
            for half in range(2):
                real = shifted[0:16, 128 * half : 128 * half + 128]
                imag = shifted[16:32, 128 * half : 128 * half + 128]
                cosine = phases[level, child, 0, 16 * half : 16 * half + 16]
                sine = phases[level, child, 1, 16 * half : 16 * half + 16]
                parts.append((real * cosine - imag * sine, real * sine + imag * cosine))
            turned.append(parts)
        return [
            tuple(turned[0][half][part] + turned[1][half][part] for part in range(2))
            for half in range(2)
        ]

    def kept(parents):
        for half in range(2):
            for part in range(2):
                held[part, 16 * half : 16 * half + 16] = parents[half][part]
        return [
            jnp.concatenate([held[part, pl.ds(child, 16, stride=2), :] for part in range(2)], axis=0)
            for child in range(2)
        ]

    for copy in blk_copies:
        copy.wait_recv()
    profiles = jnp.dot(picker, blocks[...].reshape(256, 256), preferred_element_type=F32)
    children = [
        jnp.concatenate(
            [profiles[16 * c : 16 * c + 16, 0:128], profiles[16 * c : 16 * c + 16, 128:256]], axis=0
        )
        for c in range(2)
    ]
    for level in range(4):
        children = kept(merged(level, children))
    parents = merged(4, children)

    flat_out = beams_out.reshape(64, 128)
    flat_in = beams_in.reshape(64, 128)
    for half in range(2):
        for part in range(2):
            flat_out[pl.ds(2 * half + part, 16, stride=4), :] = parents[half][part]
            flat_in[2 * half + part : 2 * half + part + 1, :] = parents[half][part][0:1]
    beam_copies = []
    for rel in (8, 9, 6, 7, 10, 11, 4, 5, 12, 13, 14, 15, 2, 3, 1):
        copy = pltpu.make_async_remote_copy(
            src_ref=beams_out.at[rel], dst_ref=beams_in.at[rel],
            send_sem=beam_send.at[rel], recv_sem=beam_recv.at[rel],
            device_id={"band": band ^ rel}, device_id_type=MESH,
        )
        copy.start()
        beam_copies.append(copy)
    for copy in beam_copies:
        copy.wait_recv()

    @pl.when(speaker)
    def _():
        pl.semaphore_wait(barrier, 31)
        for rel in range(1, 16):
            tell(all_ready, rel)

    children = [
        jnp.concatenate(
            [
                flat_in[pl.ds(4 * child + 2 * half + part, 8, stride=8), :]
                for part in range(2)
                for half in range(2)
            ],
            axis=0,
        )
        for child in range(2)
    ]
    for level in range(5, 8):
        children = kept(merged(level, children))
    parents = merged(8, children)

    @pl.when(band > 0)
    def _():
        pl.semaphore_wait(all_ready, 1)

    flat_out = rows_out.reshape(64, 128)
    flat_in = rows_in.reshape(64, 128)
    for half in range(2):
        for part in range(2):
            flat_out[pl.ds(32 * half + part, 16, stride=2), :] = parents[half][part]
    for part in range(2):
        flat_in[part : part + 1, :] = parents[0][part][0:1]
    row_copies = []
    for rel in sorted(range(1, 32), key=lambda r: -min(r & 7, 8 - (r & 7)) - min(r >> 3, 4 - (r >> 3))):
        copy = pltpu.make_async_remote_copy(
            src_ref=rows_out.at[rel], dst_ref=rows_in.at[bit_reversed(rel, 5)],
            send_sem=row_send.at[rel], recv_sem=row_recv.at[rel],
            device_id={"aperture": aperture ^ rel}, device_id_type=MESH,
        )
        copy.start()
        row_copies.append(copy)
    for copy in row_copies:
        copy.wait_recv()
    children = [
        jnp.concatenate(
            [flat_in[pl.ds(32 * child + part, 16, stride=2), :] for part in range(2)], axis=0
        )
        for child in range(2)
    ]
    for level in range(9, 13):
        parents = merged(level, children)
        for half in range(2):
            for part in range(2):
                held[part, pl.ds(half, 16, stride=2), :] = parents[half][part]
        children = [
            jnp.concatenate([held[part, 16 * child : 16 * child + 16] for part in range(2)], axis=0)
            for child in range(2)
        ]
    parents = merged(13, children)
    for half in range(2):
        padded[pl.ds(8 + half, 16, stride=2), :] = parents[half][0] ** 2 + parents[half][1] ** 2

    middle = padded[8:40]
    sums = padded[6:38]
    squares = sums * sums
    for shift in range(1, 5):
        value = padded[6 + shift : 38 + shift]
        sums = sums + value
        squares = squares + value * value
    lanes = iota((32, 128), 1)

    def across(value):
        total = value
        for shift in (1, 2):
            total = total + jnp.where(lanes >= shift, pltpu.roll(value, shift, 1), 0.0)
            total = total + jnp.where(lanes < 128 - shift, pltpu.roll(value, 128 - shift, 1), 0.0)
        return total

    count_rows = jnp.minimum(index + 2, 31) - jnp.maximum(index - 2, 0) + 1
    count_lanes = jnp.minimum(lanes + 2, 127) - jnp.maximum(lanes - 2, 0) + 1
    count = (count_rows * count_lanes).astype(F32)
    mean = across(sums) / count
    square = across(squares) / count
    gain = (square - mean * mean) / (square - 0.75 * mean * mean + 0.001)
    out_ref[...] = mean + gain * (middle - mean)

    for copy in list(core_copies.values()) + blk_copies + beam_copies + row_copies:
        copy.wait_send()


def body(raw_echoes, pulse_order, matched, offsets, fraction, tilt_angle):
    echoes = raw_echoes.reshape(512, 2, 2, 128).transpose(0, 2, 1, 3).reshape(16, 128, 128)
    dma = pltpu.SemaphoreType.DMA
    regular = pltpu.SemaphoreType.REGULAR
    return pl.pallas_call(
        kernel,
        out_shape=jax.ShapeDtypeStruct((32, 128), F32),
        in_specs=[pl.BlockSpec(memory_space=pl.ANY)] * 6,
        out_specs=pl.BlockSpec(memory_space=pltpu.VMEM),
        scratch_shapes=[
            pltpu.VMEM((1, 32), jnp.int32),
            pltpu.VMEM((2, 256), F32),
            pltpu.SMEM((2, 2, 1, LEVELS), jnp.int32),
            pltpu.SMEM((2, 2, LEVELS), F32),
            pltpu.SMEM((2, LEVELS), F32),
            pltpu.VMEM((16, 128, 128), BF16),
            pltpu.VMEM((4, 256, 128), BF16),
            pltpu.VMEM((4, 2, 512, 128), F32),
            pltpu.VMEM((8, 32, 256), F32),
            pltpu.VMEM((8, 32, 256), F32),
            pltpu.VMEM((8, 32, 256), F32),
            pltpu.VMEM((8, 32, 256), BF16),
            pltpu.VMEM((8, 32, 256), BF16),
            pltpu.VMEM((LEVELS, 2, 256, 256), BF16),
            pltpu.VMEM((LEVELS, 2, 2, 32, 128), F32),
            pltpu.VMEM((2, 32, 128), F32),
            pltpu.VMEM((16, 4, 128), F32),
            pltpu.VMEM((16, 4, 128), F32),
            pltpu.VMEM((32, 2, 128), F32),
            pltpu.VMEM((32, 2, 128), F32),
            pltpu.VMEM((48, 128), F32),
            regular, regular, regular, dma((5,)), dma((16,)), dma((8,)), dma((8,)), dma((8,)), dma((8,)),
            dma((16,)), dma((16,)), dma((32,)), dma((32,)),
        ],
        compiler_params=pltpu.CompilerParams(collective_id=0, has_side_effects=True),
    )(
        echoes,
        pulse_order.reshape(1, 32),
        matched,
        offsets.transpose(1, 2, 3, 0),
        fraction.transpose(1, 2, 0),
        tilt_angle.transpose(1, 0),
    )


def solution(mesh):
    in_specs = (P("aperture", None, "band"), P("aperture", "band", None), P(), P(), P(), P())
    out_specs = P(("band", "aperture"), None)
    return jax.shard_map(body, mesh=mesh, in_specs=in_specs, out_specs=out_specs, check_vma=False)
```

```python
import functools
import math

import jax
import jax.numpy as jnp
from jax import lax
from jax.experimental import pallas as pl
from jax.experimental.pallas import tpu as pltpu
from jax.sharding import PartitionSpec as P

LEVELS = 14
F32 = jnp.float32
BF16 = jnp.bfloat16
MESH = pl.DeviceIdType.MESH


def bit_reversed(value, bits):
    return sum(((value >> t) & 1) << (bits - 1 - t) for t in range(bits))


def sin_cos(angle):
    turns = jnp.floor(angle * (2.0 / math.pi) + 0.5)
    rest = (angle - turns * 1.5707964) - turns * (-4.371139e-08)
    sq = rest * rest
    sine = rest + rest * sq * (
        -1.0 / 6 + sq * (1.0 / 120 + sq * (-1.0 / 5040 + sq * (1.0 / 362880)))
    )
    cosine = 1.0 + sq * (-0.5 + sq * (1.0 / 24 + sq * (-1.0 / 720 + sq * (1.0 / 40320))))
    size = jnp.abs(turns)
    odd = size == 1.0
    flip = jnp.where(size == 2.0, -1.0, 1.0)
    return (
        jnp.where(odd, turns * cosine, flip * sine),
        jnp.where(odd, -turns * sine, flip * cosine),
    )


def iota(shape, dim):
    return lax.broadcasted_iota(jnp.int32, shape, dim)


def bf16_pair(value):
    high = value.astype(BF16)
    low = (value - high.astype(F32)).astype(BF16)
    return high, low


def kernel(
    x_hbm, order_hbm, matched_hbm, offs_hbm, frac_hbm, tilt_hbm, out_ref,
    order_ref, matched_ref, offs_ref, frac_ref, tilt_ref,
    xv, table, prods, own, other, from_core, partial, blocks,
    taps, phases, held, beams_out, beams_in, rows_out, rows_in, padded,
    core_ready, band_ready, all_ready, arg_sem, x_sem, core_send, core_recv, blk_send, blk_recv, beam_send, beam_recv, row_send, row_recv,
):
    band = lax.axis_index("band")
    aperture = lax.axis_index("aperture")
    parity_word = band | (aperture << 4)
    child_word = parity_word << 5

    on_first = (band & 1) == 0
    on_second = (band & 1) == 1
    speaker = band == 0
    listener = on_first & (band > 0)
    barrier = pltpu.get_barrier_semaphore()

    def greet(peer):
        pl.semaphore_signal(barrier, 1, device_id={"band": peer}, device_id_type=MESH)

    def tell(semaphore, peer):
        pl.semaphore_signal(semaphore, 1, device_id={"band": peer}, device_id_type=MESH)

    @pl.when(on_first)
    def _():
        greet(band ^ 1)

    for rel in range(2, 16, 2):
        peer = (band & 14) ^ rel

        @pl.when(peer > 0)
        def _():
            greet(peer)

    start = pl.multiple_of(band * 256, 256)
    args = [
        pltpu.make_async_copy(source, target, arg_sem.at[i])
        for i, (source, target) in enumerate(
            (
                (matched_hbm.at[:, pl.ds(start, 256)], matched_ref),
                (order_hbm, order_ref),
                (offs_hbm, offs_ref),
                (frac_hbm, frac_ref),
                (tilt_hbm, tilt_ref),
            )
        )
    ]
    args[0].start()

    loads = {}
    for pos in (4, 5, 6, 7, 0, 1, 2, 3, 12, 13, 14, 15, 8, 9, 10, 11):
        rel = 2 * pos + 1 if pos < 8 else 2 * (pos - 8)
        load = pltpu.make_async_copy(x_hbm.at[band ^ rel], xv.at[pos], x_sem.at[pos])
        load.start()
        loads[pos] = load
    for arg in args[1:]:
        arg.start()

    bins = iota((128, 128), 0).astype(F32)
    args[0].wait()
    for half in range(2):
        freq = (start + 128 * half + iota((128, 128), 1)).astype(F32)
        turns = freq * bins
        turns = turns - 4096.0 * jnp.floor(turns * (1.0 / 4096) + 0.5)
        sine, cosine = sin_cos(turns * (2.0 * math.pi / 4096))
        spec_re = matched_ref[0:1, 128 * half : 128 * half + 128]
        spec_im = matched_ref[1:2, 128 * half : 128 * half + 128]
        real = (spec_re * cosine - spec_im * sine) * (1.0 / 64)
        imag = (spec_re * sine + spec_im * cosine) * (1.0 / 64)
        table[2 * half, 0:128] = real.astype(BF16)
        table[2 * half, 128:256] = imag.astype(BF16)
        table[2 * half + 1, 0:128] = (-imag).astype(BF16)
        table[2 * half + 1, 128:256] = real.astype(BF16)

    def compress(chunk, target):
        for pos in range(4 * chunk, 4 * chunk + 4):
            loads[pos].wait()
        echoes = xv[4 * chunk : 4 * chunk + 4].reshape(512, 128)
        for kind in range(4):
            prod = lax.dot_general(
                echoes, table[kind], (((1,), (1,)), ((), ())), preferred_element_type=F32
            )
            prods[kind, 0] = prod[:, 0:128]
            prods[kind, 1] = prod[:, 128:256]
        base = 4 * (chunk % 2)
        for part in range(2):
            total = prods[0, part, pl.ds(0, 128, stride=4), :]
            for kind in range(1, 4):
                total = total + prods[kind, part, pl.ds(kind, 128, stride=4), :]
            target[base : base + 4, :, 128 * part : 128 * part + 128] = total.reshape(4, 32, 128)

    order_far = (4, 3, 5, 2, 6, 7, 1, 0)
    core_copies = {}

    def to_partner(slots):
        for j in slots:
            copy = pltpu.make_async_remote_copy(
                src_ref=other.at[j], dst_ref=from_core.at[j],
                send_sem=core_send.at[j], recv_sem=core_recv.at[j],
                device_id={"band": band ^ 1}, device_id_type=MESH,
            )
            copy.start()
            core_copies[j] = copy

    compress(1, other)

    @pl.when(on_second)
    def _():
        pl.semaphore_wait(barrier, 1)
        tell(core_ready, band ^ 1)

    @pl.when(on_first)
    def _():
        pl.semaphore_wait(core_ready, 1)

    to_partner((4, 5, 6, 7))
    compress(0, other)
    to_partner((3, 2, 1, 0))
    compress(3, own)
    compress(2, own)

    @pl.when(listener)
    def _():
        pl.semaphore_wait(barrier, 14)
        tell(band_ready, band ^ 1)

    @pl.when(band == 2)
    def _():
        tell(band_ready, 0)

    @pl.when(speaker)
    def _():
        pl.semaphore_wait(band_ready, 1)
        tell(band_ready, 1)
        for rel in range(1, 32):
            pl.semaphore_signal(
                barrier, 1, device_id={"aperture": aperture ^ rel}, device_id_type=MESH
            )

    @pl.when(on_second)
    def _():
        pl.semaphore_wait(band_ready, 1)

    blk_copies = []
    for j in order_far:
        core_copies[j].wait_recv()
        summed = (own[j] + from_core[j]).astype(BF16)
        if j == 0:
            blocks[0] = summed
            continue
        partial[j] = summed
        copy = pltpu.make_async_remote_copy(
            src_ref=partial.at[j], dst_ref=blocks.at[j],
            send_sem=blk_send.at[j], recv_sem=blk_recv.at[j],
            device_id={"band": band ^ (2 * j)}, device_id_type=MESH,
        )
        copy.start()
        blk_copies.append(copy)

    for arg in args[1:]:
        arg.wait()
    lane = iota((8, 128), 1)
    signed_lane = jnp.where(lane < 64, lane, lane - 128)
    lane8 = lane
    row8 = iota((8, 128), 0)

    @pl.loop(0, LEVELS)
    def _(level):
        parity_flip = (parity_word >> level) & 1
        child_flip = (child_word >> level) & 1
        for child in range(2):
            for half in range(2):
                offset = offs_ref[child ^ child_flip, half ^ parity_flip, 0, level]
                shift = frac_ref[child ^ child_flip, half ^ parity_flip, level]
                whole = 8 - offset - signed_lane
                dist = whole.astype(F32) - shift
                fracs = jnp.full((8, 128), math.pi, F32) * shift
                sq = fracs * fracs
                sine = fracs * (1.0 + sq * (-1.0 / 6 + sq * (1.0 / 120 + sq * (-1.0 / 5040 + sq * (1.0 / 362880 - sq * (1.0 / 39916800))))))
                sine = jnp.where((whole & 1) == 0, -sine, sine)
                zero = dist == 0.0
                sinc = jnp.where(zero, 1.0, sine / jnp.where(zero, 1.0, dist * math.pi))
                scaled = dist * (1.0 / 2.5)
                weight = sinc * jnp.exp(-(scaled * scaled)) * math.sqrt(0.5)
                weight = jnp.where(jnp.abs(dist) <= 4.0, weight, 0.0)
                strips = []
                for strip in range(16):
                    turned = pltpu.roll(weight, 8 * strip, 1, stride=1, stride_axis=0)
                    source = row8 + 8 * strip
                    window = source + 8 - offset
                    keep = (jnp.abs(lane8 - source) < 64) & (window >= 0) & (window < 128)
                    strips.append(jnp.where(keep, turned, 0.0))
                matrix = jnp.concatenate(strips, axis=0)
                high, low = bf16_pair(matrix)
                taps[level, child, 0:128, 128 * half : 128 * half + 128] = high
                taps[level, child, 128:256, 128 * half : 128 * half + 128] = low

    index = iota((32, 128), 0)
    row = index & 15
    half_bit = index >> 4
    for level in range(LEVELS):
        beam = half_bit ^ ((parity_word >> level) & 1)
        for t in range(level):
            if level <= 4 or (level <= 8 and t >= 4):
                bit = ((row >> (4 - level + t)) & 1) ^ ((parity_word >> t) & 1)
            elif t >= 9:
                bit = (row >> (level - 1 - t)) & 1
            else:
                bit = (parity_word >> t) & 1
            beam = beam + (bit << (level - t))
        position = 2.0 * (beam.astype(F32) + 0.5) / 2.0 ** (level + 1) - 1.0
        for child in range(2):
            angle = tilt_ref[child ^ ((child_word >> level) & 1), level] * position
            sine, cosine = sin_cos(angle)
            phases[level, child, 0] = cosine
            phases[level, child, 1] = sine

    padded[...] = jnp.zeros_like(padded)

    place = iota((32, 32), 0)
    pulse = ((place & 15) << 1) | (place >> 4)
    order = jnp.broadcast_to(order_ref[0:1, :].astype(F32), (32, 32))
    column = jnp.sum(jnp.where(iota((32, 32), 1) == pulse, order, 0.0), axis=1, keepdims=True)
    chosen = (iota((32, 256), 1) & 31).astype(F32)
    picker = jnp.where(chosen == column, 1.0, 0.0).astype(BF16)

    def merged(level, children):
        turned = []
        for child in range(2):
            high, low = bf16_pair(children[child])
            left = jnp.concatenate(
                [jnp.concatenate([high, high], axis=1), jnp.concatenate([low, low], axis=1)], axis=0
            )
            both = jnp.dot(left, taps[level, child], preferred_element_type=F32)
            shifted = both[0:32] + both[32:64]
            parts = []
            for half in range(2):
                real = shifted[0:16, 128 * half : 128 * half + 128]
                imag = shifted[16:32, 128 * half : 128 * half + 128]
                cosine = phases[level, child, 0, 16 * half : 16 * half + 16]
                sine = phases[level, child, 1, 16 * half : 16 * half + 16]
                parts.append((real * cosine - imag * sine, real * sine + imag * cosine))
            turned.append(parts)
        return [
            tuple(turned[0][half][part] + turned[1][half][part] for part in range(2))
            for half in range(2)
        ]

    def kept(parents):
        for half in range(2):
            for part in range(2):
                held[part, 16 * half : 16 * half + 16] = parents[half][part]
        return [
            jnp.concatenate([held[part, pl.ds(child, 16, stride=2), :] for part in range(2)], axis=0)
            for child in range(2)
        ]

    for copy in blk_copies:
        copy.wait_recv()
    profiles = jnp.dot(picker, blocks[...].reshape(256, 256), preferred_element_type=F32)
    children = [
        jnp.concatenate(
            [profiles[16 * c : 16 * c + 16, 0:128], profiles[16 * c : 16 * c + 16, 128:256]], axis=0
        )
        for c in range(2)
    ]
    for level in range(4):
        children = kept(merged(level, children))
    parents = merged(4, children)

    flat_out = beams_out.reshape(64, 128)
    flat_in = beams_in.reshape(64, 128)
    for half in range(2):
        for part in range(2):
            flat_out[pl.ds(2 * half + part, 16, stride=4), :] = parents[half][part]
            flat_in[2 * half + part : 2 * half + part + 1, :] = parents[half][part][0:1]
    beam_copies = []
    for rel in (8, 9, 6, 7, 10, 11, 4, 5, 12, 13, 14, 15, 2, 3, 1):
        copy = pltpu.make_async_remote_copy(
            src_ref=beams_out.at[rel], dst_ref=beams_in.at[rel],
            send_sem=beam_send.at[rel], recv_sem=beam_recv.at[rel],
            device_id={"band": band ^ rel}, device_id_type=MESH,
        )
        copy.start()
        beam_copies.append(copy)
    @pl.when(speaker)
    def _():
        pl.semaphore_wait(barrier, 31)
        for rel in range(1, 16):
            tell(all_ready, rel)

    for copy in beam_copies:
        copy.wait_recv()
    children = [
        jnp.concatenate(
            [
                flat_in[pl.ds(4 * child + 2 * half + part, 8, stride=8), :]
                for part in range(2)
                for half in range(2)
            ],
            axis=0,
        )
        for child in range(2)
    ]
    for level in range(5, 8):
        children = kept(merged(level, children))
    parents = merged(8, children)

    @pl.when(band > 0)
    def _():
        pl.semaphore_wait(all_ready, 1)

    flat_out = rows_out.reshape(64, 128)
    flat_in = rows_in.reshape(64, 128)
    for half in range(2):
        for part in range(2):
            flat_out[pl.ds(32 * half + part, 16, stride=2), :] = parents[half][part]
    for part in range(2):
        flat_in[part : part + 1, :] = parents[0][part][0:1]
    row_copies = []
    for rel in sorted(range(1, 32), key=lambda r: -min(r & 7, 8 - (r & 7)) - min(r >> 3, 4 - (r >> 3))):
        copy = pltpu.make_async_remote_copy(
            src_ref=rows_out.at[rel], dst_ref=rows_in.at[bit_reversed(rel, 5)],
            send_sem=row_send.at[rel], recv_sem=row_recv.at[rel],
            device_id={"aperture": aperture ^ rel}, device_id_type=MESH,
        )
        copy.start()
        row_copies.append(copy)
    for copy in row_copies:
        copy.wait_recv()
    children = [
        jnp.concatenate(
            [flat_in[pl.ds(32 * child + part, 16, stride=2), :] for part in range(2)], axis=0
        )
        for child in range(2)
    ]
    for level in range(9, 13):
        parents = merged(level, children)
        for half in range(2):
            for part in range(2):
                held[part, pl.ds(half, 16, stride=2), :] = parents[half][part]
        children = [
            jnp.concatenate([held[part, 16 * child : 16 * child + 16] for part in range(2)], axis=0)
            for child in range(2)
        ]
    parents = merged(13, children)
    for half in range(2):
        padded[pl.ds(8 + half, 16, stride=2), :] = parents[half][0] ** 2 + parents[half][1] ** 2

    middle = padded[8:40]
    sums = padded[6:38]
    squares = sums * sums
    for shift in range(1, 5):
        value = padded[6 + shift : 38 + shift]
        sums = sums + value
        squares = squares + value * value
    lanes = iota((32, 128), 1)

    def across(value):
        total = value
        for shift in (1, 2):
            total = total + jnp.where(lanes >= shift, pltpu.roll(value, shift, 1), 0.0)
            total = total + jnp.where(lanes < 128 - shift, pltpu.roll(value, 128 - shift, 1), 0.0)
        return total

    count_rows = jnp.minimum(index + 2, 31) - jnp.maximum(index - 2, 0) + 1
    count_lanes = jnp.minimum(lanes + 2, 127) - jnp.maximum(lanes - 2, 0) + 1
    count = (count_rows * count_lanes).astype(F32)
    mean = across(sums) / count
    square = across(squares) / count
    gain = (square - mean * mean) / (square - 0.75 * mean * mean + 0.001)
    out_ref[...] = mean + gain * (middle - mean)

    for copy in list(core_copies.values()) + blk_copies + beam_copies + row_copies:
        copy.wait_send()


def body(raw_echoes, pulse_order, matched, offsets, fraction, tilt_angle):
    echoes = raw_echoes.reshape(512, 2, 2, 128).transpose(0, 2, 1, 3).reshape(16, 128, 128)
    dma = pltpu.SemaphoreType.DMA
    regular = pltpu.SemaphoreType.REGULAR
    return pl.pallas_call(
        kernel,
        out_shape=pltpu.VMEM((32, 128), F32),
        in_specs=[pl.BlockSpec(memory_space=pl.ANY)] * 6,
        out_specs=pl.BlockSpec(memory_space=pltpu.VMEM),
        scratch_shapes=[
            pltpu.VMEM((1, 32), jnp.int32),
            pltpu.VMEM((2, 256), F32),
            pltpu.SMEM((2, 2, 1, LEVELS), jnp.int32),
            pltpu.SMEM((2, 2, LEVELS), F32),
            pltpu.SMEM((2, LEVELS), F32),
            pltpu.VMEM((16, 128, 128), BF16),
            pltpu.VMEM((4, 256, 128), BF16),
            pltpu.VMEM((4, 2, 512, 128), F32),
            pltpu.VMEM((8, 32, 256), F32),
            pltpu.VMEM((8, 32, 256), F32),
            pltpu.VMEM((8, 32, 256), F32),
            pltpu.VMEM((8, 32, 256), BF16),
            pltpu.VMEM((8, 32, 256), BF16),
            pltpu.VMEM((LEVELS, 2, 256, 256), BF16),
            pltpu.VMEM((LEVELS, 2, 2, 32, 128), F32),
            pltpu.VMEM((2, 32, 128), F32),
            pltpu.VMEM((16, 4, 128), F32),
            pltpu.VMEM((16, 4, 128), F32),
            pltpu.VMEM((32, 2, 128), F32),
            pltpu.VMEM((32, 2, 128), F32),
            pltpu.VMEM((48, 128), F32),
            regular, regular, regular, dma((5,)), dma((16,)), dma((8,)), dma((8,)), dma((8,)), dma((8,)),
            dma((16,)), dma((16,)), dma((32,)), dma((32,)),
        ],
        compiler_params=pltpu.CompilerParams(collective_id=0, has_side_effects=True),
    )(
        echoes,
        pulse_order.reshape(1, 32),
        matched,
        offsets.transpose(1, 2, 3, 0),
        fraction.transpose(1, 2, 0),
        tilt_angle.transpose(1, 0),
    )


def solution(mesh):
    in_specs = (P("aperture", None, "band"), P("aperture", "band", None), P(), P(), P(), P())
    out_specs = P(("band", "aperture"), None)
    return jax.shard_map(body, mesh=mesh, in_specs=in_specs, out_specs=out_specs, check_vma=False)
```

```python
import functools
import math

import jax
import jax.numpy as jnp
from jax import lax
from jax.experimental import pallas as pl
from jax.experimental.pallas import tpu as pltpu
from jax.sharding import PartitionSpec as P

LEVELS = 14
F32 = jnp.float32
BF16 = jnp.bfloat16
MESH = pl.DeviceIdType.MESH


def bit_reversed(value, bits):
    return sum(((value >> t) & 1) << (bits - 1 - t) for t in range(bits))


def sin_cos(angle):
    turns = jnp.floor(angle * (2.0 / math.pi) + 0.5)
    rest = (angle - turns * 1.5707964) - turns * (-4.371139e-08)
    sq = rest * rest
    sine = rest + rest * sq * (
        -1.0 / 6 + sq * (1.0 / 120 + sq * (-1.0 / 5040 + sq * (1.0 / 362880)))
    )
    cosine = 1.0 + sq * (-0.5 + sq * (1.0 / 24 + sq * (-1.0 / 720 + sq * (1.0 / 40320))))
    size = jnp.abs(turns)
    odd = size == 1.0
    flip = jnp.where(size == 2.0, -1.0, 1.0)
    return (
        jnp.where(odd, turns * cosine, flip * sine),
        jnp.where(odd, -turns * sine, flip * cosine),
    )


def iota(shape, dim):
    return lax.broadcasted_iota(jnp.int32, shape, dim)


def bf16_pair(value):
    high = value.astype(BF16)
    low = (value - high.astype(F32)).astype(BF16)
    return high, low


def kernel(
    x_hbm, order_hbm, matched_hbm, offs_hbm, frac_hbm, tilt_hbm, out_ref,
    order_ref, matched_ref, offs_ref, frac_ref, tilt_ref,
    xv, table, prods, own, other, from_core, partial, blocks,
    taps, phases, held, beams_out, beams_in, rows_out, rows_in, padded,
    core_ready, band_ready, all_ready, arg_sem, x_sem, core_send, core_recv, blk_send, blk_recv, beam_send, beam_recv, row_send, row_recv,
):
    band = lax.axis_index("band")
    aperture = lax.axis_index("aperture")
    parity_word = band | (aperture << 4)
    child_word = parity_word << 5

    on_first = (band & 1) == 0
    on_second = (band & 1) == 1
    speaker = band == 0
    listener = on_first & (band > 0)
    barrier = pltpu.get_barrier_semaphore()

    def greet(peer):
        pl.semaphore_signal(barrier, 1, device_id={"band": peer}, device_id_type=MESH)

    def tell(semaphore, peer):
        pl.semaphore_signal(semaphore, 1, device_id={"band": peer}, device_id_type=MESH)

    @pl.when(on_first)
    def _():
        greet(band ^ 1)

    for rel in range(2, 16, 2):
        peer = (band & 14) ^ rel

        @pl.when(peer > 0)
        def _():
            greet(peer)

    start = pl.multiple_of(band * 256, 256)
    args = [
        pltpu.make_async_copy(source, target, arg_sem.at[i])
        for i, (source, target) in enumerate(
            (
                (matched_hbm.at[:, pl.ds(start, 256)], matched_ref),
                (order_hbm, order_ref),
                (offs_hbm, offs_ref),
                (frac_hbm, frac_ref),
                (tilt_hbm, tilt_ref),
            )
        )
    ]
    args[0].start()

    loads = {}
    for pos in (4, 5, 6, 7, 0, 1, 2, 3, 12, 13, 14, 15, 8, 9, 10, 11):
        rel = 2 * pos + 1 if pos < 8 else 2 * (pos - 8)
        for half in range(2):
            load = pltpu.make_async_copy(
                x_hbm.at[band ^ rel, :, half], xv.at[half, pos], x_sem.at[half, pos]
            )
            load.start()
            loads[half, pos] = load
    for arg in args[1:]:
        arg.start()

    @pl.when(on_second)
    def _():
        pl.semaphore_wait(barrier, 1)
        tell(core_ready, band ^ 1)

    bins = iota((128, 128), 0).astype(F32)
    args[0].wait()
    for half in range(2):
        freq = (start + 128 * half + iota((128, 128), 1)).astype(F32)
        turns = freq * bins
        turns = turns - 4096.0 * jnp.floor(turns * (1.0 / 4096) + 0.5)
        sine, cosine = sin_cos(turns * (2.0 * math.pi / 4096))
        spec_re = matched_ref[0:1, 128 * half : 128 * half + 128]
        spec_im = matched_ref[1:2, 128 * half : 128 * half + 128]
        real = (spec_re * cosine - spec_im * sine) * (1.0 / 64)
        imag = (spec_re * sine + spec_im * cosine) * (1.0 / 64)
        side = slice(128 * half, 128 * half + 128)
        table[0, 0:128, side] = real.astype(BF16)
        table[0, 128:256, side] = imag.astype(BF16)
        table[1, 0:128, side] = (-imag).astype(BF16)
        table[1, 128:256, side] = real.astype(BF16)

    def compress(chunk, target):
        for pos in range(4 * chunk, 4 * chunk + 4):
            for half in range(2):
                loads[half, pos].wait()
        echoes = jnp.concatenate(
            [xv.at[half].reshape(1024, 128)[256 * chunk : 256 * chunk + 256] for half in range(2)],
            axis=1,
        )
        for part in range(2):
            prod = lax.dot_general(
                echoes, table[part], (((1,), (1,)), ((), ())), preferred_element_type=F32
            )
            prods[part, 0] = prod[:, 0:128]
            prods[part, 1] = prod[:, 128:256]
        base = 4 * (chunk % 2)
        for out in range(2):
            total = prods[0, out, pl.ds(0, 128, stride=2), :] + prods[1, out, pl.ds(1, 128, stride=2), :]
            target[base : base + 4, :, 128 * out : 128 * out + 128] = total.reshape(4, 32, 128)

    order_far = (4, 3, 5, 2, 6, 7, 1, 0)
    core_copies = {}

    def to_partner(slots):
        for j in slots:
            copy = pltpu.make_async_remote_copy(
                src_ref=other.at[j], dst_ref=from_core.at[j],
                send_sem=core_send.at[j], recv_sem=core_recv.at[j],
                device_id={"band": band ^ 1}, device_id_type=MESH,
            )
            copy.start()
            core_copies[j] = copy

    compress(1, other)

    @pl.when(on_first)
    def _():
        pl.semaphore_wait(core_ready, 1)

    to_partner((4, 5, 6, 7))
    compress(0, other)
    to_partner((3, 2, 1, 0))
    compress(3, own)

    @pl.when(listener)
    def _():
        pl.semaphore_wait(barrier, 14)

    @pl.when(band == 2)
    def _():
        tell(band_ready, 0)

    @pl.when(listener)
    def _():
        tell(band_ready, band ^ 1)

    compress(2, own)

    @pl.when(speaker)
    def _():
        pl.semaphore_wait(band_ready, 1)
        tell(band_ready, 1)
        for rel in range(1, 32):
            pl.semaphore_signal(
                barrier, 1, device_id={"aperture": aperture ^ rel}, device_id_type=MESH
            )

    @pl.when(on_second)
    def _():
        pl.semaphore_wait(band_ready, 1)

    blk_copies = []
    for j in order_far:
        core_copies[j].wait_recv()
        summed = (own[j] + from_core[j]).astype(BF16)
        if j == 0:
            blocks[0] = summed
            continue
        partial[j] = summed
        copy = pltpu.make_async_remote_copy(
            src_ref=partial.at[j], dst_ref=blocks.at[j],
            send_sem=blk_send.at[j], recv_sem=blk_recv.at[j],
            device_id={"band": band ^ (2 * j)}, device_id_type=MESH,
        )
        copy.start()
        blk_copies.append(copy)

    for arg in args[1:]:
        arg.wait()
    lane = iota((8, 128), 1)
    signed_lane = jnp.where(lane < 64, lane, lane - 128)
    lane8 = lane
    row8 = iota((8, 128), 0)

    @pl.loop(0, LEVELS)
    def _(level):
        parity_flip = (parity_word >> level) & 1
        child_flip = (child_word >> level) & 1
        for child in range(2):
            for half in range(2):
                offset = offs_ref[child ^ child_flip, half ^ parity_flip, 0, level]
                shift = frac_ref[child ^ child_flip, half ^ parity_flip, level]
                whole = 8 - offset - signed_lane
                dist = whole.astype(F32) - shift
                fracs = jnp.full((8, 128), math.pi, F32) * shift
                sq = fracs * fracs
                sine = fracs * (1.0 + sq * (-1.0 / 6 + sq * (1.0 / 120 + sq * (-1.0 / 5040 + sq * (1.0 / 362880 - sq * (1.0 / 39916800))))))
                sine = jnp.where((whole & 1) == 0, -sine, sine)
                zero = dist == 0.0
                sinc = jnp.where(zero, 1.0, sine / jnp.where(zero, 1.0, dist * math.pi))
                scaled = dist * (1.0 / 2.5)
                weight = sinc * jnp.exp(-(scaled * scaled)) * math.sqrt(0.5)
                weight = jnp.where(jnp.abs(dist) <= 4.0, weight, 0.0)
                strips = []
                for strip in range(16):
                    turned = pltpu.roll(weight, 8 * strip, 1, stride=1, stride_axis=0)
                    source = row8 + 8 * strip
                    window = source + 8 - offset
                    keep = (jnp.abs(lane8 - source) < 64) & (window >= 0) & (window < 128)
                    strips.append(jnp.where(keep, turned, 0.0))
                matrix = jnp.concatenate(strips, axis=0)
                high, low = bf16_pair(matrix)
                taps[level, child, 0:128, 128 * half : 128 * half + 128] = high
                taps[level, child, 128:256, 128 * half : 128 * half + 128] = low

    index = iota((32, 128), 0)
    row = index & 15
    half_bit = index >> 4
    for level in range(LEVELS):
        beam = half_bit ^ ((parity_word >> level) & 1)
        for t in range(level):
            if level <= 4 or (level <= 8 and t >= 4):
                bit = ((row >> (4 - level + t)) & 1) ^ ((parity_word >> t) & 1)
            elif t >= 9:
                bit = (row >> (level - 1 - t)) & 1
            else:
                bit = (parity_word >> t) & 1
            beam = beam + (bit << (level - t))
        position = 2.0 * (beam.astype(F32) + 0.5) / 2.0 ** (level + 1) - 1.0
        for child in range(2):
            angle = tilt_ref[child ^ ((child_word >> level) & 1), level] * position
            sine, cosine = sin_cos(angle)
            phases[level, child, 0] = cosine
            phases[level, child, 1] = sine

    padded[...] = jnp.zeros_like(padded)

    place = iota((32, 32), 0)
    pulse = ((place & 15) << 1) | (place >> 4)
    order = jnp.broadcast_to(order_ref[0:1, :].astype(F32), (32, 32))
    column = jnp.sum(jnp.where(iota((32, 32), 1) == pulse, order, 0.0), axis=1, keepdims=True)
    chosen = (iota((32, 256), 1) & 31).astype(F32)
    picker = jnp.where(chosen == column, 1.0, 0.0).astype(BF16)

    def merged(level, children):
        turned = []
        for child in range(2):
            high, low = bf16_pair(children[child])
            left = jnp.concatenate(
                [jnp.concatenate([high, high], axis=1), jnp.concatenate([low, low], axis=1)], axis=0
            )
            both = jnp.dot(left, taps[level, child], preferred_element_type=F32)
            shifted = both[0:32] + both[32:64]
            parts = []
            for half in range(2):
                real = shifted[0:16, 128 * half : 128 * half + 128]
                imag = shifted[16:32, 128 * half : 128 * half + 128]
                cosine = phases[level, child, 0, 16 * half : 16 * half + 16]
                sine = phases[level, child, 1, 16 * half : 16 * half + 16]
                parts.append((real * cosine - imag * sine, real * sine + imag * cosine))
            turned.append(parts)
        return [
            tuple(turned[0][half][part] + turned[1][half][part] for part in range(2))
            for half in range(2)
        ]

    def kept(parents):
        for half in range(2):
            for part in range(2):
                held[part, 16 * half : 16 * half + 16] = parents[half][part]
        return [
            jnp.concatenate([held[part, pl.ds(child, 16, stride=2), :] for part in range(2)], axis=0)
            for child in range(2)
        ]

    for copy in blk_copies:
        copy.wait_recv()
    profiles = jnp.dot(picker, blocks[...].reshape(256, 256), preferred_element_type=F32)
    children = [
        jnp.concatenate(
            [profiles[16 * c : 16 * c + 16, 0:128], profiles[16 * c : 16 * c + 16, 128:256]], axis=0
        )
        for c in range(2)
    ]
    for level in range(4):
        children = kept(merged(level, children))
    parents = merged(4, children)

    flat_out = beams_out.reshape(64, 128)
    flat_in = beams_in.reshape(64, 128)
    for half in range(2):
        for part in range(2):
            flat_out[pl.ds(2 * half + part, 16, stride=4), :] = parents[half][part]
            flat_in[2 * half + part : 2 * half + part + 1, :] = parents[half][part][0:1]
    beam_copies = []
    for rel in (8, 9, 6, 7, 10, 11, 4, 5, 12, 13, 14, 15, 2, 3, 1):
        copy = pltpu.make_async_remote_copy(
            src_ref=beams_out.at[rel], dst_ref=beams_in.at[rel],
            send_sem=beam_send.at[rel], recv_sem=beam_recv.at[rel],
            device_id={"band": band ^ rel}, device_id_type=MESH,
        )
        copy.start()
        beam_copies.append(copy)
    @pl.when(speaker)
    def _():
        pl.semaphore_wait(barrier, 31)
        for rel in range(1, 16):
            tell(all_ready, rel)

    for copy in beam_copies:
        copy.wait_recv()
    children = [
        jnp.concatenate(
            [
                flat_in[pl.ds(4 * child + 2 * half + part, 8, stride=8), :]
                for part in range(2)
                for half in range(2)
            ],
            axis=0,
        )
        for child in range(2)
    ]
    for level in range(5, 8):
        children = kept(merged(level, children))
    parents = merged(8, children)

    @pl.when(band > 0)
    def _():
        pl.semaphore_wait(all_ready, 1)

    flat_out = rows_out.reshape(64, 128)
    flat_in = rows_in.reshape(64, 128)
    for half in range(2):
        for part in range(2):
            flat_out[pl.ds(32 * half + part, 16, stride=2), :] = parents[half][part]
    for part in range(2):
        flat_in[part : part + 1, :] = parents[0][part][0:1]
    row_copies = []
    for rel in sorted(range(1, 32), key=lambda r: (-(r & 4), -min(r & 7, 8 - (r & 7)) - min(r >> 3, 4 - (r >> 3)))):
        copy = pltpu.make_async_remote_copy(
            src_ref=rows_out.at[rel], dst_ref=rows_in.at[bit_reversed(rel, 5)],
            send_sem=row_send.at[rel], recv_sem=row_recv.at[rel],
            device_id={"aperture": aperture ^ rel}, device_id_type=MESH,
        )
        copy.start()
        row_copies.append(copy)
    for copy in row_copies:
        copy.wait_recv()
    children = [
        jnp.concatenate(
            [flat_in[pl.ds(32 * child + part, 16, stride=2), :] for part in range(2)], axis=0
        )
        for child in range(2)
    ]
    for level in range(9, 13):
        parents = merged(level, children)
        for half in range(2):
            for part in range(2):
                held[part, pl.ds(half, 16, stride=2), :] = parents[half][part]
        children = [
            jnp.concatenate([held[part, 16 * child : 16 * child + 16] for part in range(2)], axis=0)
            for child in range(2)
        ]
    parents = merged(13, children)
    for half in range(2):
        padded[pl.ds(8 + half, 16, stride=2), :] = parents[half][0] ** 2 + parents[half][1] ** 2

    middle = padded[8:40]
    sums = padded[6:38]
    squares = sums * sums
    for shift in range(1, 5):
        value = padded[6 + shift : 38 + shift]
        sums = sums + value
        squares = squares + value * value
    lanes = iota((32, 128), 1)

    def across(value):
        total = value
        for shift in (1, 2):
            total = total + jnp.where(lanes >= shift, pltpu.roll(value, shift, 1), 0.0)
            total = total + jnp.where(lanes < 128 - shift, pltpu.roll(value, 128 - shift, 1), 0.0)
        return total

    count_rows = jnp.minimum(index + 2, 31) - jnp.maximum(index - 2, 0) + 1
    count_lanes = jnp.minimum(lanes + 2, 127) - jnp.maximum(lanes - 2, 0) + 1
    count = (count_rows * count_lanes).astype(F32)
    mean = across(sums) / count
    square = across(squares) / count
    gain = (square - mean * mean) / (square - 0.75 * mean * mean + 0.001)
    out_ref[...] = mean + gain * (middle - mean)

    for copy in list(core_copies.values()) + blk_copies + beam_copies + row_copies:
        copy.wait_send()


def body(raw_echoes, pulse_order, matched, offsets, fraction, tilt_angle):
    echoes = raw_echoes.reshape(512, 2, 2, 128).transpose(0, 2, 1, 3).reshape(16, 32, 2, 2, 128)
    dma = pltpu.SemaphoreType.DMA
    regular = pltpu.SemaphoreType.REGULAR
    return pl.pallas_call(
        kernel,
        out_shape=pltpu.VMEM((32, 128), F32),
        in_specs=[pl.BlockSpec(memory_space=pl.ANY)] * 6,
        out_specs=pl.BlockSpec(memory_space=pltpu.VMEM),
        scratch_shapes=[
            pltpu.VMEM((1, 32), jnp.int32),
            pltpu.VMEM((2, 256), F32),
            pltpu.SMEM((2, 2, 1, LEVELS), jnp.int32),
            pltpu.SMEM((2, 2, LEVELS), F32),
            pltpu.SMEM((2, LEVELS), F32),
            pltpu.VMEM((2, 16, 32, 2, 128), BF16),
            pltpu.VMEM((2, 256, 256), BF16),
            pltpu.VMEM((2, 2, 256, 128), F32),
            pltpu.VMEM((8, 32, 256), F32),
            pltpu.VMEM((8, 32, 256), F32),
            pltpu.VMEM((8, 32, 256), F32),
            pltpu.VMEM((8, 32, 256), BF16),
            pltpu.VMEM((8, 32, 256), BF16),
            pltpu.VMEM((LEVELS, 2, 256, 256), BF16),
            pltpu.VMEM((LEVELS, 2, 2, 32, 128), F32),
            pltpu.VMEM((2, 32, 128), F32),
            pltpu.VMEM((16, 4, 128), F32),
            pltpu.VMEM((16, 4, 128), F32),
            pltpu.VMEM((32, 2, 128), F32),
            pltpu.VMEM((32, 2, 128), F32),
            pltpu.VMEM((48, 128), F32),
            regular, regular, regular, dma((5,)), dma((2, 16)), dma((8,)), dma((8,)), dma((8,)), dma((8,)),
            dma((16,)), dma((16,)), dma((32,)), dma((32,)),
        ],
        compiler_params=pltpu.CompilerParams(collective_id=0, has_side_effects=True),
    )(
        echoes,
        pulse_order.reshape(1, 32),
        matched,
        offsets.transpose(1, 2, 3, 0),
        fraction.transpose(1, 2, 0),
        tilt_angle.transpose(1, 0),
    )


def solution(mesh):
    in_specs = (P("aperture", None, "band"), P("aperture", "band", None), P(), P(), P(), P())
    out_specs = P(("band", "aperture"), None)
    return jax.shard_map(body, mesh=mesh, in_specs=in_specs, out_specs=out_specs, check_vma=False)
```

```python
import functools
import math

import jax
import jax.numpy as jnp
from jax import lax
from jax.experimental import pallas as pl
from jax.experimental.pallas import tpu as pltpu
from jax.sharding import PartitionSpec as P

LEVELS = 14
F32 = jnp.float32
BF16 = jnp.bfloat16
MESH = pl.DeviceIdType.MESH


def bit_reversed(value, bits):
    return sum(((value >> t) & 1) << (bits - 1 - t) for t in range(bits))


def sin_cos(angle):
    turns = jnp.floor(angle * (2.0 / math.pi) + 0.5)
    rest = (angle - turns * 1.5707964) - turns * (-4.371139e-08)
    sq = rest * rest
    sine = rest + rest * sq * (
        -1.0 / 6 + sq * (1.0 / 120 + sq * (-1.0 / 5040 + sq * (1.0 / 362880)))
    )
    cosine = 1.0 + sq * (-0.5 + sq * (1.0 / 24 + sq * (-1.0 / 720 + sq * (1.0 / 40320))))
    size = jnp.abs(turns)
    odd = size == 1.0
    flip = jnp.where(size == 2.0, -1.0, 1.0)
    return (
        jnp.where(odd, turns * cosine, flip * sine),
        jnp.where(odd, -turns * sine, flip * cosine),
    )


def iota(shape, dim):
    return lax.broadcasted_iota(jnp.int32, shape, dim)


def bf16_pair(value):
    high = value.astype(BF16)
    low = (value - high.astype(F32)).astype(BF16)
    return high, low


def kernel(
    x_hbm, order_hbm, matched_hbm, offs_hbm, frac_hbm, tilt_hbm, out_ref,
    order_ref, matched_ref, offs_ref, frac_ref, tilt_ref,
    xv, table, prods, own, other, from_core, partial, blocks,
    taps, phases, held, beams_out, beams_in, rows_out, rows_in, padded,
    core_ready, band_ready, all_ready, arg_sem, x_sem, core_send, core_recv, blk_send, blk_recv, beam_send, beam_recv, row_send, row_recv,
):
    band = lax.axis_index("band")
    aperture = lax.axis_index("aperture")
    parity_word = band | (aperture << 4)
    child_word = parity_word << 5

    on_first = (band & 1) == 0
    on_second = (band & 1) == 1
    speaker = band == 0
    listener = on_first & (band > 0)
    barrier = pltpu.get_barrier_semaphore()

    def greet(peer):
        pl.semaphore_signal(barrier, 1, device_id={"band": peer}, device_id_type=MESH)

    def tell(semaphore, peer):
        pl.semaphore_signal(semaphore, 1, device_id={"band": peer}, device_id_type=MESH)

    @pl.when(on_first)
    def _():
        greet(band ^ 1)

    for rel in range(2, 16, 2):
        peer = (band & 14) ^ rel

        @pl.when(peer > 0)
        def _():
            greet(peer)

    start = pl.multiple_of(band * 256, 256)
    args = [
        pltpu.make_async_copy(source, target, arg_sem.at[i])
        for i, (source, target) in enumerate(
            (
                (matched_hbm.at[:, pl.ds(start, 256)], matched_ref),
                (order_hbm, order_ref),
                (offs_hbm, offs_ref),
                (frac_hbm, frac_ref),
                (tilt_hbm, tilt_ref),
            )
        )
    ]
    args[0].start()

    loads = {}
    for pos in (4, 5, 6, 7, 0, 1, 2, 3, 12, 13, 14, 15, 8, 9, 10, 11):
        rel = 2 * pos + 1 if pos < 8 else 2 * (pos - 8)
        for half in range(2):
            load = pltpu.make_async_copy(
                x_hbm.at[band ^ rel, :, half], xv.at[half, pos], x_sem.at[half, pos]
            )
            load.start()
            loads[half, pos] = load
    for arg in args[1:]:
        arg.start()

    bins = iota((128, 128), 0).astype(F32)
    args[0].wait()
    for half in range(2):
        freq = (start + 128 * half + iota((128, 128), 1)).astype(F32)
        turns = freq * bins
        turns = turns - 4096.0 * jnp.floor(turns * (1.0 / 4096) + 0.5)
        sine, cosine = sin_cos(turns * (2.0 * math.pi / 4096))
        spec_re = matched_ref[0:1, 128 * half : 128 * half + 128]
        spec_im = matched_ref[1:2, 128 * half : 128 * half + 128]
        real = (spec_re * cosine - spec_im * sine) * (1.0 / 64)
        imag = (spec_re * sine + spec_im * cosine) * (1.0 / 64)
        side = slice(128 * half, 128 * half + 128)
        table[0, 0:128, side] = real.astype(BF16)
        table[0, 128:256, side] = imag.astype(BF16)
        table[1, 0:128, side] = (-imag).astype(BF16)
        table[1, 128:256, side] = real.astype(BF16)

    def compress(chunk, target):
        for pos in range(4 * chunk, 4 * chunk + 4):
            for half in range(2):
                loads[half, pos].wait()
        echoes = jnp.concatenate(
            [xv.at[half].reshape(1024, 128)[256 * chunk : 256 * chunk + 256] for half in range(2)],
            axis=1,
        )
        for part in range(2):
            prod = lax.dot_general(
                echoes, table[part], (((1,), (1,)), ((), ())), preferred_element_type=F32
            )
            prods[part, 0] = prod[:, 0:128]
            prods[part, 1] = prod[:, 128:256]
        base = 4 * (chunk % 2)
        for out in range(2):
            total = prods[0, out, pl.ds(0, 128, stride=2), :] + prods[1, out, pl.ds(1, 128, stride=2), :]
            target[base : base + 4, :, 128 * out : 128 * out + 128] = total.reshape(4, 32, 128)

    order_far = (4, 3, 5, 2, 6, 7, 1, 0)
    core_copies = {}

    def to_partner(slots):
        for j in slots:
            copy = pltpu.make_async_remote_copy(
                src_ref=other.at[j], dst_ref=from_core.at[j],
                send_sem=core_send.at[j], recv_sem=core_recv.at[j],
                device_id={"band": band ^ 1}, device_id_type=MESH,
            )
            copy.start()
            core_copies[j] = copy

    compress(1, other)

    @pl.when(on_second)
    def _():
        pl.semaphore_wait(barrier, 1)
        tell(core_ready, band ^ 1)

    @pl.when(on_first)
    def _():
        pl.semaphore_wait(core_ready, 1)

    to_partner((4, 5, 6, 7))
    compress(0, other)
    to_partner((3, 2, 1, 0))
    compress(3, own)
    compress(2, own)

    @pl.when(listener)
    def _():
        pl.semaphore_wait(barrier, 14)
        tell(band_ready, band ^ 1)

    @pl.when(band == 2)
    def _():
        tell(band_ready, 0)

    @pl.when(speaker)
    def _():
        pl.semaphore_wait(band_ready, 1)
        tell(band_ready, 1)
        for rel in range(1, 32):
            pl.semaphore_signal(
                barrier, 1, device_id={"aperture": aperture ^ rel}, device_id_type=MESH
            )

    @pl.when(on_second)
    def _():
        pl.semaphore_wait(band_ready, 1)

    blk_copies = []
    for j in order_far:
        core_copies[j].wait_recv()
        summed = (own[j] + from_core[j]).astype(BF16)
        if j == 0:
            blocks[0] = summed
            continue
        partial[j] = summed
        copy = pltpu.make_async_remote_copy(
            src_ref=partial.at[j], dst_ref=blocks.at[j],
            send_sem=blk_send.at[j], recv_sem=blk_recv.at[j],
            device_id={"band": band ^ (2 * j)}, device_id_type=MESH,
        )
        copy.start()
        blk_copies.append(copy)

    for arg in args[1:]:
        arg.wait()
    lane = iota((8, 128), 1)
    signed_lane = jnp.where(lane < 64, lane, lane - 128)
    lane8 = lane
    row8 = iota((8, 128), 0)

    @pl.loop(0, LEVELS)
    def _(level):
        parity_flip = (parity_word >> level) & 1
        child_flip = (child_word >> level) & 1
        for child in range(2):
            for half in range(2):
                offset = offs_ref[child ^ child_flip, half ^ parity_flip, 0, level]
                shift = frac_ref[child ^ child_flip, half ^ parity_flip, level]
                whole = 8 - offset - signed_lane
                dist = whole.astype(F32) - shift
                fracs = jnp.full((8, 128), math.pi, F32) * shift
                sq = fracs * fracs
                sine = fracs * (1.0 + sq * (-1.0 / 6 + sq * (1.0 / 120 + sq * (-1.0 / 5040 + sq * (1.0 / 362880 - sq * (1.0 / 39916800))))))
                sine = jnp.where((whole & 1) == 0, -sine, sine)
                zero = dist == 0.0
                sinc = jnp.where(zero, 1.0, sine / jnp.where(zero, 1.0, dist * math.pi))
                scaled = dist * (1.0 / 2.5)
                weight = sinc * jnp.exp(-(scaled * scaled)) * math.sqrt(0.5)
                weight = jnp.where(jnp.abs(dist) <= 4.0, weight, 0.0)
                strips = []
                for strip in range(16):
                    turned = pltpu.roll(weight, 8 * strip, 1, stride=1, stride_axis=0)
                    source = row8 + 8 * strip
                    window = source + 8 - offset
                    keep = (jnp.abs(lane8 - source) < 64) & (window >= 0) & (window < 128)
                    strips.append(jnp.where(keep, turned, 0.0))
                matrix = jnp.concatenate(strips, axis=0)
                high, low = bf16_pair(matrix)
                taps[level, child, 0:128, 128 * half : 128 * half + 128] = high
                taps[level, child, 128:256, 128 * half : 128 * half + 128] = low

    index = iota((32, 128), 0)
    row = index & 15
    half_bit = index >> 4
    for level in range(LEVELS):
        beam = half_bit ^ ((parity_word >> level) & 1)
        for t in range(level):
            if level <= 4 or (level <= 8 and t >= 4):
                bit = ((row >> (4 - level + t)) & 1) ^ ((parity_word >> t) & 1)
            elif t >= 9:
                bit = (row >> (level - 1 - t)) & 1
            else:
                bit = (parity_word >> t) & 1
            beam = beam + (bit << (level - t))
        position = 2.0 * (beam.astype(F32) + 0.5) / 2.0 ** (level + 1) - 1.0
        for child in range(2):
            angle = tilt_ref[child ^ ((child_word >> level) & 1), level] * position
            sine, cosine = sin_cos(angle)
            phases[level, child, 0] = cosine
            phases[level, child, 1] = sine

    padded[...] = jnp.zeros_like(padded)

    place = iota((32, 32), 0)
    pulse = ((place & 15) << 1) | (place >> 4)
    order = jnp.broadcast_to(order_ref[0:1, :].astype(F32), (32, 32))
    column = jnp.sum(jnp.where(iota((32, 32), 1) == pulse, order, 0.0), axis=1, keepdims=True)
    chosen = (iota((32, 256), 1) & 31).astype(F32)
    picker = jnp.where(chosen == column, 1.0, 0.0).astype(BF16)

    def merged(level, children):
        turned = []
        for child in range(2):
            high, low = bf16_pair(children[child])
            left = jnp.concatenate(
                [jnp.concatenate([high, high], axis=1), jnp.concatenate([low, low], axis=1)], axis=0
            )
            both = jnp.dot(left, taps[level, child], preferred_element_type=F32)
            shifted = both[0:32] + both[32:64]
            parts = []
            for half in range(2):
                real = shifted[0:16, 128 * half : 128 * half + 128]
                imag = shifted[16:32, 128 * half : 128 * half + 128]
                cosine = phases[level, child, 0, 16 * half : 16 * half + 16]
                sine = phases[level, child, 1, 16 * half : 16 * half + 16]
                parts.append((real * cosine - imag * sine, real * sine + imag * cosine))
            turned.append(parts)
        return [
            tuple(turned[0][half][part] + turned[1][half][part] for part in range(2))
            for half in range(2)
        ]

    def kept(parents):
        for half in range(2):
            for part in range(2):
                held[part, 16 * half : 16 * half + 16] = parents[half][part]
        return [
            jnp.concatenate([held[part, pl.ds(child, 16, stride=2), :] for part in range(2)], axis=0)
            for child in range(2)
        ]

    for copy in blk_copies:
        copy.wait_recv()
    profiles = jnp.dot(picker, blocks[...].reshape(256, 256), preferred_element_type=F32)
    children = [
        jnp.concatenate(
            [profiles[16 * c : 16 * c + 16, 0:128], profiles[16 * c : 16 * c + 16, 128:256]], axis=0
        )
        for c in range(2)
    ]
    for level in range(4):
        children = kept(merged(level, children))
    parents = merged(4, children)

    flat_out = beams_out.reshape(64, 128)
    flat_in = beams_in.reshape(64, 128)
    for half in range(2):
        for part in range(2):
            flat_out[pl.ds(2 * half + part, 16, stride=4), :] = parents[half][part]
            flat_in[2 * half + part : 2 * half + part + 1, :] = parents[half][part][0:1]
    beam_copies = []
    for rel in (8, 9, 6, 7, 10, 11, 4, 5, 12, 13, 14, 15, 2, 3, 1):
        copy = pltpu.make_async_remote_copy(
            src_ref=beams_out.at[rel], dst_ref=beams_in.at[rel],
            send_sem=beam_send.at[rel], recv_sem=beam_recv.at[rel],
            device_id={"band": band ^ rel}, device_id_type=MESH,
        )
        copy.start()
        beam_copies.append(copy)
    @pl.when(speaker)
    def _():
        pl.semaphore_wait(barrier, 31)
        for rel in range(1, 16):
            tell(all_ready, rel)

    for copy in beam_copies:
        copy.wait_recv()
    children = [
        jnp.concatenate(
            [
                flat_in[pl.ds(4 * child + 2 * half + part, 8, stride=8), :]
                for part in range(2)
                for half in range(2)
            ],
            axis=0,
        )
        for child in range(2)
    ]
    for level in range(5, 8):
        children = kept(merged(level, children))
    parents = merged(8, children)

    @pl.when(band > 0)
    def _():
        pl.semaphore_wait(all_ready, 1)

    flat_out = rows_out.reshape(64, 128)
    flat_in = rows_in.reshape(64, 128)
    for half in range(2):
        for part in range(2):
            flat_out[pl.ds(32 * half + part, 16, stride=2), :] = parents[half][part]
    for part in range(2):
        flat_in[part : part + 1, :] = parents[0][part][0:1]
    row_copies = []
    for rel in sorted(range(1, 32), key=lambda r: -min(r & 7, 8 - (r & 7)) - min(r >> 3, 4 - (r >> 3))):
        copy = pltpu.make_async_remote_copy(
            src_ref=rows_out.at[rel], dst_ref=rows_in.at[bit_reversed(rel, 5)],
            send_sem=row_send.at[rel], recv_sem=row_recv.at[rel],
            device_id={"aperture": aperture ^ rel}, device_id_type=MESH,
        )
        copy.start()
        row_copies.append(copy)
    for copy in row_copies:
        copy.wait_recv()
    children = [
        jnp.concatenate(
            [flat_in[pl.ds(32 * child + part, 16, stride=2), :] for part in range(2)], axis=0
        )
        for child in range(2)
    ]
    for level in range(9, 13):
        parents = merged(level, children)
        for half in range(2):
            for part in range(2):
                held[part, pl.ds(half, 16, stride=2), :] = parents[half][part]
        children = [
            jnp.concatenate([held[part, 16 * child : 16 * child + 16] for part in range(2)], axis=0)
            for child in range(2)
        ]
    parents = merged(13, children)
    for half in range(2):
        padded[pl.ds(8 + half, 16, stride=2), :] = parents[half][0] ** 2 + parents[half][1] ** 2

    middle = padded[8:40]
    sums = padded[6:38]
    squares = sums * sums
    for shift in range(1, 5):
        value = padded[6 + shift : 38 + shift]
        sums = sums + value
        squares = squares + value * value
    lanes = iota((32, 128), 1)

    def across(value):
        total = value
        for shift in (1, 2):
            total = total + jnp.where(lanes >= shift, pltpu.roll(value, shift, 1), 0.0)
            total = total + jnp.where(lanes < 128 - shift, pltpu.roll(value, 128 - shift, 1), 0.0)
        return total

    count_rows = jnp.minimum(index + 2, 31) - jnp.maximum(index - 2, 0) + 1
    count_lanes = jnp.minimum(lanes + 2, 127) - jnp.maximum(lanes - 2, 0) + 1
    count = (count_rows * count_lanes).astype(F32)
    mean = across(sums) / count
    square = across(squares) / count
    gain = (square - mean * mean) / (square - 0.75 * mean * mean + 0.001)
    out_ref[...] = mean + gain * (middle - mean)

    for copy in list(core_copies.values()) + blk_copies + beam_copies + row_copies:
        copy.wait_send()


def body(raw_echoes, pulse_order, matched, offsets, fraction, tilt_angle):
    echoes = raw_echoes.reshape(512, 2, 2, 128).transpose(0, 2, 1, 3).reshape(16, 32, 2, 2, 128)
    dma = pltpu.SemaphoreType.DMA
    regular = pltpu.SemaphoreType.REGULAR
    return pl.pallas_call(
        kernel,
        out_shape=pltpu.VMEM((32, 128), F32),
        in_specs=[pl.BlockSpec(memory_space=pl.ANY)] * 6,
        out_specs=pl.BlockSpec(memory_space=pltpu.VMEM),
        scratch_shapes=[
            pltpu.VMEM((1, 32), jnp.int32),
            pltpu.VMEM((2, 256), F32),
            pltpu.SMEM((2, 2, 1, LEVELS), jnp.int32),
            pltpu.SMEM((2, 2, LEVELS), F32),
            pltpu.SMEM((2, LEVELS), F32),
            pltpu.VMEM((2, 16, 32, 2, 128), BF16),
            pltpu.VMEM((2, 256, 256), BF16),
            pltpu.VMEM((2, 2, 256, 128), F32),
            pltpu.VMEM((8, 32, 256), F32),
            pltpu.VMEM((8, 32, 256), F32),
            pltpu.VMEM((8, 32, 256), F32),
            pltpu.VMEM((8, 32, 256), BF16),
            pltpu.VMEM((8, 32, 256), BF16),
            pltpu.VMEM((LEVELS, 2, 256, 256), BF16),
            pltpu.VMEM((LEVELS, 2, 2, 32, 128), F32),
            pltpu.VMEM((2, 32, 128), F32),
            pltpu.VMEM((16, 4, 128), F32),
            pltpu.VMEM((16, 4, 128), F32),
            pltpu.VMEM((32, 2, 128), F32),
            pltpu.VMEM((32, 2, 128), F32),
            pltpu.VMEM((48, 128), F32),
            regular, regular, regular, dma((5,)), dma((2, 16)), dma((8,)), dma((8,)), dma((8,)), dma((8,)),
            dma((16,)), dma((16,)), dma((32,)), dma((32,)),
        ],
        compiler_params=pltpu.CompilerParams(collective_id=0, has_side_effects=True),
    )(
        echoes,
        pulse_order.reshape(1, 32),
        matched,
        offsets.transpose(1, 2, 3, 0),
        fraction.transpose(1, 2, 0),
        tilt_angle.transpose(1, 0),
    )


def solution(mesh):
    in_specs = (P("aperture", None, "band"), P("aperture", "band", None), P(), P(), P(), P())
    out_specs = P(("band", "aperture"), None)
    return jax.shard_map(body, mesh=mesh, in_specs=in_specs, out_specs=out_specs, check_vma=False)
```

```python
import functools
import math

import jax
import jax.numpy as jnp
from jax import lax
from jax.experimental import pallas as pl
from jax.experimental.pallas import tpu as pltpu
from jax.sharding import PartitionSpec as P

LEVELS = 14
F32 = jnp.float32
BF16 = jnp.bfloat16
MESH = pl.DeviceIdType.MESH


def bit_reversed(value, bits):
    return sum(((value >> t) & 1) << (bits - 1 - t) for t in range(bits))


def sin_cos(angle):
    turns = jnp.floor(angle * (2.0 / math.pi) + 0.5)
    rest = (angle - turns * 1.5707964) - turns * (-4.371139e-08)
    sq = rest * rest
    sine = rest + rest * sq * (
        -1.0 / 6 + sq * (1.0 / 120 + sq * (-1.0 / 5040 + sq * (1.0 / 362880)))
    )
    cosine = 1.0 + sq * (-0.5 + sq * (1.0 / 24 + sq * (-1.0 / 720 + sq * (1.0 / 40320))))
    size = jnp.abs(turns)
    odd = size == 1.0
    flip = jnp.where(size == 2.0, -1.0, 1.0)
    return (
        jnp.where(odd, turns * cosine, flip * sine),
        jnp.where(odd, -turns * sine, flip * cosine),
    )


def iota(shape, dim):
    return lax.broadcasted_iota(jnp.int32, shape, dim)


def bf16_pair(value):
    high = value.astype(BF16)
    low = (value - high.astype(F32)).astype(BF16)
    return high, low


def kernel(
    x_hbm, order_hbm, matched_hbm, offs_hbm, frac_hbm, tilt_hbm, out_ref,
    order_ref, matched_ref, offs_ref, frac_ref, tilt_ref,
    xv, table, prods, own, other, from_core, partial, blocks,
    taps, phases, held, beams_out, beams_in, rows_out, rows_in, padded,
    core_ready, band_ready, all_ready, arg_sem, x_sem, core_send, core_recv, blk_send, blk_recv, beam_send, beam_recv, row_send, row_recv,
):
    band = lax.axis_index("band")
    aperture = lax.axis_index("aperture")
    parity_word = band | (aperture << 4)
    child_word = parity_word << 5

    on_first = (band & 1) == 0
    on_second = (band & 1) == 1
    speaker = band == 0
    listener = on_first & (band > 0)
    barrier = pltpu.get_barrier_semaphore()

    def greet(peer):
        pl.semaphore_signal(barrier, 1, device_id={"band": peer}, device_id_type=MESH)

    def tell(semaphore, peer):
        pl.semaphore_signal(semaphore, 1, device_id={"band": peer}, device_id_type=MESH)

    @pl.when(on_first)
    def _():
        greet(band ^ 1)

    for rel in range(2, 16, 2):
        peer = (band & 14) ^ rel

        @pl.when(peer > 0)
        def _():
            greet(peer)

    start = pl.multiple_of(band * 256, 256)
    args = [
        pltpu.make_async_copy(source, target, arg_sem.at[i])
        for i, (source, target) in enumerate(
            (
                (matched_hbm.at[:, pl.ds(start, 256)], matched_ref),
                (order_hbm, order_ref),
                (offs_hbm, offs_ref),
                (frac_hbm, frac_ref),
                (tilt_hbm, tilt_ref),
            )
        )
    ]
    args[0].start()

    loads = {}
    for pos in (4, 5, 6, 7, 0, 1, 2, 3, 12, 13, 14, 15, 8, 9, 10, 11):
        rel = 2 * pos + 1 if pos < 8 else 2 * (pos - 8)
        load = pltpu.make_async_copy(x_hbm.at[band ^ rel], xv.at[pos], x_sem.at[pos])
        load.start()
        loads[pos] = load
    for arg in args[1:]:
        arg.start()

    @pl.when(on_second)
    def _():
        pl.semaphore_wait(barrier, 1)
        tell(core_ready, band ^ 1)

    bins = iota((128, 128), 0).astype(F32)
    args[0].wait()
    for half in range(2):
        freq = (start + 128 * half + iota((128, 128), 1)).astype(F32)
        turns = freq * bins
        turns = turns - 4096.0 * jnp.floor(turns * (1.0 / 4096) + 0.5)
        sine, cosine = sin_cos(turns * (2.0 * math.pi / 4096))
        spec_re = matched_ref[0:1, 128 * half : 128 * half + 128]
        spec_im = matched_ref[1:2, 128 * half : 128 * half + 128]
        real = (spec_re * cosine - spec_im * sine) * (1.0 / 64)
        imag = (spec_re * sine + spec_im * cosine) * (1.0 / 64)
        table[2 * half, 0:128] = real.astype(BF16)
        table[2 * half, 128:256] = imag.astype(BF16)
        table[2 * half + 1, 0:128] = (-imag).astype(BF16)
        table[2 * half + 1, 128:256] = real.astype(BF16)

    def compress(chunk, target):
        for pos in range(4 * chunk, 4 * chunk + 4):
            loads[pos].wait()
        echoes = xv[4 * chunk : 4 * chunk + 4].reshape(512, 128)
        for kind in range(4):
            prod = lax.dot_general(
                echoes, table[kind], (((1,), (1,)), ((), ())), preferred_element_type=F32
            )
            prods[kind, 0] = prod[:, 0:128]
            prods[kind, 1] = prod[:, 128:256]
        base = 4 * (chunk % 2)
        for part in range(2):
            total = prods[0, part, pl.ds(0, 128, stride=4), :]
            for kind in range(1, 4):
                total = total + prods[kind, part, pl.ds(kind, 128, stride=4), :]
            target[base : base + 4, :, 128 * part : 128 * part + 128] = total.reshape(4, 32, 128)

    order_far = (4, 3, 5, 2, 6, 7, 1, 0)
    core_copies = {}

    def to_partner(slots):
        for j in slots:
            copy = pltpu.make_async_remote_copy(
                src_ref=other.at[j], dst_ref=from_core.at[j],
                send_sem=core_send.at[j], recv_sem=core_recv.at[j],
                device_id={"band": band ^ 1}, device_id_type=MESH,
            )
            copy.start()
            core_copies[j] = copy

    compress(1, other)

    @pl.when(on_first)
    def _():
        pl.semaphore_wait(core_ready, 1)

    to_partner((4, 5, 6, 7))
    compress(0, other)
    to_partner((3, 2, 1, 0))
    compress(3, own)
    compress(2, own)

    @pl.when(listener)
    def _():
        pl.semaphore_wait(barrier, 14)
        tell(band_ready, band ^ 1)

    @pl.when(band == 2)
    def _():
        tell(band_ready, 0)

    @pl.when(speaker)
    def _():
        pl.semaphore_wait(band_ready, 1)
        tell(band_ready, 1)
        for rel in range(1, 32):
            pl.semaphore_signal(
                barrier, 1, device_id={"aperture": aperture ^ rel}, device_id_type=MESH
            )

    @pl.when(on_second)
    def _():
        pl.semaphore_wait(band_ready, 1)

    blk_copies = []
    for j in order_far:
        core_copies[j].wait_recv()
        summed = (own[j] + from_core[j]).astype(BF16)
        if j == 0:
            blocks[0] = summed
            continue
        partial[j] = summed
        copy = pltpu.make_async_remote_copy(
            src_ref=partial.at[j], dst_ref=blocks.at[j],
            send_sem=blk_send.at[j], recv_sem=blk_recv.at[j],
            device_id={"band": band ^ (2 * j)}, device_id_type=MESH,
        )
        copy.start()
        blk_copies.append(copy)

    for arg in args[1:]:
        arg.wait()
    lane = iota((8, 128), 1)
    signed_lane = jnp.where(lane < 64, lane, lane - 128)
    lane8 = lane
    row8 = iota((8, 128), 0)

    @pl.loop(0, LEVELS)
    def _(level):
        parity_flip = (parity_word >> level) & 1
        child_flip = (child_word >> level) & 1
        for child in range(2):
            for half in range(2):
                offset = offs_ref[child ^ child_flip, half ^ parity_flip, 0, level]
                shift = frac_ref[child ^ child_flip, half ^ parity_flip, level]
                whole = 8 - offset - signed_lane
                dist = whole.astype(F32) - shift
                fracs = jnp.full((8, 128), math.pi, F32) * shift
                sq = fracs * fracs
                sine = fracs * (1.0 + sq * (-1.0 / 6 + sq * (1.0 / 120 + sq * (-1.0 / 5040 + sq * (1.0 / 362880 - sq * (1.0 / 39916800))))))
                sine = jnp.where((whole & 1) == 0, -sine, sine)
                zero = dist == 0.0
                sinc = jnp.where(zero, 1.0, sine / jnp.where(zero, 1.0, dist * math.pi))
                scaled = dist * (1.0 / 2.5)
                weight = sinc * jnp.exp(-(scaled * scaled)) * math.sqrt(0.5)
                weight = jnp.where(jnp.abs(dist) <= 4.0, weight, 0.0)
                strips = []
                for strip in range(16):
                    turned = pltpu.roll(weight, 8 * strip, 1, stride=1, stride_axis=0)
                    source = row8 + 8 * strip
                    window = source + 8 - offset
                    keep = (jnp.abs(lane8 - source) < 64) & (window >= 0) & (window < 128)
                    strips.append(jnp.where(keep, turned, 0.0))
                matrix = jnp.concatenate(strips, axis=0)
                high, low = bf16_pair(matrix)
                taps[level, child, 0:128, 128 * half : 128 * half + 128] = high
                taps[level, child, 128:256, 128 * half : 128 * half + 128] = low

    index = iota((32, 128), 0)
    row = index & 15
    half_bit = index >> 4
    for level in range(LEVELS):
        beam = half_bit ^ ((parity_word >> level) & 1)
        for t in range(level):
            if level <= 4 or (level <= 8 and t >= 4):
                bit = ((row >> (4 - level + t)) & 1) ^ ((parity_word >> t) & 1)
            elif t >= 9:
                bit = (row >> (level - 1 - t)) & 1
            else:
                bit = (parity_word >> t) & 1
            beam = beam + (bit << (level - t))
        position = 2.0 * (beam.astype(F32) + 0.5) / 2.0 ** (level + 1) - 1.0
        for child in range(2):
            angle = tilt_ref[child ^ ((child_word >> level) & 1), level] * position
            sine, cosine = sin_cos(angle)
            phases[level, child, 0] = cosine
            phases[level, child, 1] = sine

    padded[...] = jnp.zeros_like(padded)

    place = iota((32, 32), 0)
    pulse = ((place & 15) << 1) | (place >> 4)
    order = jnp.broadcast_to(order_ref[0:1, :].astype(F32), (32, 32))
    column = jnp.sum(jnp.where(iota((32, 32), 1) == pulse, order, 0.0), axis=1, keepdims=True)
    chosen = (iota((32, 256), 1) & 31).astype(F32)
    picker = jnp.where(chosen == column, 1.0, 0.0).astype(BF16)

    def merged(level, children):
        turned = []
        for child in range(2):
            high, low = bf16_pair(children[child])
            left = jnp.concatenate(
                [jnp.concatenate([high, high], axis=1), jnp.concatenate([low, low], axis=1)], axis=0
            )
            both = jnp.dot(left, taps[level, child], preferred_element_type=F32)
            shifted = both[0:32] + both[32:64]
            parts = []
            for half in range(2):
                real = shifted[0:16, 128 * half : 128 * half + 128]
                imag = shifted[16:32, 128 * half : 128 * half + 128]
                cosine = phases[level, child, 0, 16 * half : 16 * half + 16]
                sine = phases[level, child, 1, 16 * half : 16 * half + 16]
                parts.append((real * cosine - imag * sine, real * sine + imag * cosine))
            turned.append(parts)
        return [
            tuple(turned[0][half][part] + turned[1][half][part] for part in range(2))
            for half in range(2)
        ]

    def kept(parents):
        for half in range(2):
            for part in range(2):
                held[part, 16 * half : 16 * half + 16] = parents[half][part]
        return [
            jnp.concatenate([held[part, pl.ds(child, 16, stride=2), :] for part in range(2)], axis=0)
            for child in range(2)
        ]

    for copy in blk_copies:
        copy.wait_recv()
    profiles = jnp.dot(picker, blocks[...].reshape(256, 256), preferred_element_type=F32)
    children = [
        jnp.concatenate(
            [profiles[16 * c : 16 * c + 16, 0:128], profiles[16 * c : 16 * c + 16, 128:256]], axis=0
        )
        for c in range(2)
    ]
    for level in range(4):
        children = kept(merged(level, children))
    parents = merged(4, children)

    flat_out = beams_out.reshape(64, 128)
    flat_in = beams_in.reshape(64, 128)
    for half in range(2):
        for part in range(2):
            flat_out[pl.ds(2 * half + part, 16, stride=4), :] = parents[half][part]
            flat_in[2 * half + part : 2 * half + part + 1, :] = parents[half][part][0:1]
    beam_copies = []
    for rel in (8, 9, 6, 7, 10, 11, 4, 5, 12, 13, 14, 15, 2, 3, 1):
        copy = pltpu.make_async_remote_copy(
            src_ref=beams_out.at[rel], dst_ref=beams_in.at[rel],
            send_sem=beam_send.at[rel], recv_sem=beam_recv.at[rel],
            device_id={"band": band ^ rel}, device_id_type=MESH,
        )
        copy.start()
        beam_copies.append(copy)
    @pl.when(speaker)
    def _():
        pl.semaphore_wait(barrier, 31)
        for rel in range(1, 16):
            tell(all_ready, rel)

    for copy in beam_copies:
        copy.wait_recv()
    children = [
        jnp.concatenate(
            [
                flat_in[pl.ds(4 * child + 2 * half + part, 8, stride=8), :]
                for part in range(2)
                for half in range(2)
            ],
            axis=0,
        )
        for child in range(2)
    ]
    for level in range(5, 8):
        children = kept(merged(level, children))
    parents = merged(8, children)

    @pl.when(band > 0)
    def _():
        pl.semaphore_wait(all_ready, 1)

    flat_out = rows_out.reshape(64, 128)
    flat_in = rows_in.reshape(64, 128)
    for half in range(2):
        for part in range(2):
            flat_out[pl.ds(32 * half + part, 16, stride=2), :] = parents[half][part]
    for part in range(2):
        flat_in[part : part + 1, :] = parents[0][part][0:1]
    row_copies = []
    for rel in sorted(range(1, 32), key=lambda r: -min(r & 7, 8 - (r & 7)) - min(r >> 3, 4 - (r >> 3))):
        copy = pltpu.make_async_remote_copy(
            src_ref=rows_out.at[rel], dst_ref=rows_in.at[bit_reversed(rel, 5)],
            send_sem=row_send.at[rel], recv_sem=row_recv.at[rel],
            device_id={"aperture": aperture ^ rel}, device_id_type=MESH,
        )
        copy.start()
        row_copies.append(copy)
    for copy in row_copies:
        copy.wait_recv()
    children = [
        jnp.concatenate(
            [flat_in[pl.ds(32 * child + part, 16, stride=2), :] for part in range(2)], axis=0
        )
        for child in range(2)
    ]
    for level in range(9, 13):
        parents = merged(level, children)
        for half in range(2):
            for part in range(2):
                held[part, pl.ds(half, 16, stride=2), :] = parents[half][part]
        children = [
            jnp.concatenate([held[part, 16 * child : 16 * child + 16] for part in range(2)], axis=0)
            for child in range(2)
        ]
    parents = merged(13, children)
    for half in range(2):
        padded[pl.ds(8 + half, 16, stride=2), :] = parents[half][0] ** 2 + parents[half][1] ** 2

    middle = padded[8:40]
    sums = padded[6:38]
    squares = sums * sums
    for shift in range(1, 5):
        value = padded[6 + shift : 38 + shift]
        sums = sums + value
        squares = squares + value * value
    lanes = iota((32, 128), 1)

    def across(value):
        total = value
        for shift in (1, 2):
            total = total + jnp.where(lanes >= shift, pltpu.roll(value, shift, 1), 0.0)
            total = total + jnp.where(lanes < 128 - shift, pltpu.roll(value, 128 - shift, 1), 0.0)
        return total

    count_rows = jnp.minimum(index + 2, 31) - jnp.maximum(index - 2, 0) + 1
    count_lanes = jnp.minimum(lanes + 2, 127) - jnp.maximum(lanes - 2, 0) + 1
    count = (count_rows * count_lanes).astype(F32)
    mean = across(sums) / count
    square = across(squares) / count
    gain = (square - mean * mean) / (square - 0.75 * mean * mean + 0.001)
    out_ref[...] = mean + gain * (middle - mean)

    for copy in list(core_copies.values()) + blk_copies + beam_copies + row_copies:
        copy.wait_send()


def body(raw_echoes, pulse_order, matched, offsets, fraction, tilt_angle):
    echoes = raw_echoes.reshape(512, 2, 2, 128).transpose(0, 2, 1, 3).reshape(16, 128, 128)
    dma = pltpu.SemaphoreType.DMA
    regular = pltpu.SemaphoreType.REGULAR
    return pl.pallas_call(
        kernel,
        out_shape=pltpu.VMEM((32, 128), F32),
        in_specs=[pl.BlockSpec(memory_space=pl.ANY)] * 6,
        out_specs=pl.BlockSpec(memory_space=pltpu.VMEM),
        scratch_shapes=[
            pltpu.VMEM((1, 32), jnp.int32),
            pltpu.VMEM((2, 256), F32),
            pltpu.SMEM((2, 2, 1, LEVELS), jnp.int32),
            pltpu.SMEM((2, 2, LEVELS), F32),
            pltpu.SMEM((2, LEVELS), F32),
            pltpu.VMEM((16, 128, 128), BF16),
            pltpu.VMEM((4, 256, 128), BF16),
            pltpu.VMEM((4, 2, 512, 128), F32),
            pltpu.VMEM((8, 32, 256), F32),
            pltpu.VMEM((8, 32, 256), F32),
            pltpu.VMEM((8, 32, 256), F32),
            pltpu.VMEM((8, 32, 256), BF16),
            pltpu.VMEM((8, 32, 256), BF16),
            pltpu.VMEM((LEVELS, 2, 256, 256), BF16),
            pltpu.VMEM((LEVELS, 2, 2, 32, 128), F32),
            pltpu.VMEM((2, 32, 128), F32),
            pltpu.VMEM((16, 4, 128), F32),
            pltpu.VMEM((16, 4, 128), F32),
            pltpu.VMEM((32, 2, 128), F32),
            pltpu.VMEM((32, 2, 128), F32),
            pltpu.VMEM((48, 128), F32),
            regular, regular, regular, dma((5,)), dma((16,)), dma((8,)), dma((8,)), dma((8,)), dma((8,)),
            dma((16,)), dma((16,)), dma((32,)), dma((32,)),
        ],
        compiler_params=pltpu.CompilerParams(collective_id=0, has_side_effects=True),
    )(
        echoes,
        pulse_order.reshape(1, 32),
        matched,
        offsets.transpose(1, 2, 3, 0),
        fraction.transpose(1, 2, 0),
        tilt_angle.transpose(1, 0),
    )


def solution(mesh):
    in_specs = (P("aperture", None, "band"), P("aperture", "band", None), P(), P(), P(), P())
    out_specs = P(("band", "aperture"), None)
    return jax.shard_map(body, mesh=mesh, in_specs=in_specs, out_specs=out_specs, check_vma=False)
```
